512 devices in a mesh: gx: 8 (over z), gy: 4 (over x_lo, core), gz: 16 (over y, x_hi).
Axes of the slice: x: 4 (x_hi: 2, x_lo: 2; x = x_hi * 2 + x_lo), y: 8, z: 8, core: 2. Of those that a mesh axis runs over, the one named last changes fastest.
Arguments:
- probe_bits: int32 [32, 128, 512], P('gx', 'gz', 'gy'), may hold values from -2147483648 to 2147483646
- disorder_levels: int32 [32, 128, 512], P('gx', 'gz', 'gy'), may hold values from -2147483648 to 2147483647, as said below
Outputs:
- moments: float32 [3, 8], replicated
- previous: float32 [8, 32, 512, 512], P(None, 'gx', 'gz', 'gy')
- current: float32 [8, 32, 512, 512], P(None, 'gx', 'gz', 'gy')
The draws below stay inside these ranges and needn't reach their ends.
Inputs may be any that keep to these rules, and one draw needn't show every extreme that they name: `disorder_levels`: every byte of a word is a level 0 to 255.
All inputs are finite; a program needn't handle non-finite values.
Results may differ from the reference program's by a relative error of at most 0.00002.
Values sent between devices are 32-bit elements; how exact they have to be, the bound alone decides.
No kernel may reach another device: no remote copies, remote signals or barrier semaphores. Data moves between devices by JAX's collectives and lax.ppermute only.
A program may use at most 64 MiB of HBM per device.

```python
import jax
import jax.numpy as jnp
from jax import lax

PROBES = 8
LEVELS = 256
NX = 32
NY = 512
NZ = 512
NSITES = 8388608


def draw_disorder_levels(key, part):
    shape = (NX, NZ, NY)
    group = jax.random.randint(jax.random.fold_in(key, 11), (), 0, 2)
    base = 32 + jax.random.randint(jax.random.fold_in(key, 12), (), 0, 64) + 128 * group
    slope = 32 * (2 * jax.random.randint(jax.random.fold_in(key, 13), (), 0, 2) - 1)
    offsets = jax.random.randint(jax.random.fold_in(key, 14), (4, 4, 4), -16, 17)
    widths = jax.random.randint(jax.random.fold_in(key, 15), (4, 4, 4), 16, 80)
    patch_x = lax.broadcasted_iota(jnp.int32, shape, 0) * 4 // NX
    patch_z = lax.broadcasted_iota(jnp.int32, shape, 1) * 4 // NZ
    patch_y = lax.broadcasted_iota(jnp.int32, shape, 2) * 4 // NY
    local_offset = offsets[patch_x, patch_z, patch_y]
    local_width = widths[patch_x, patch_z, patch_y]
    centre = base + slope * (patch_x - 1) + local_offset
    raw = jax.random.randint(jax.random.fold_in(key, 16), shape, 0, 161)
    jitter = raw % (2 * local_width + 1) - local_width
    patchy = jnp.clip(centre + jitter, 0, LEVELS - 1)
    background = jax.random.randint(jax.random.fold_in(key, 17), shape, 0, LEVELS)
    picker = jax.random.randint(jax.random.fold_in(key, 18), shape, 0, 8)
    levels = jnp.where(picker == 0, background, patchy).astype(jnp.int32)
    grouped = levels.reshape(NX, NZ // 4, 4, NY)
    top_byte = grouped[:, :, 3, :]
    top_signed = jnp.where(top_byte >= 128, top_byte - 256, top_byte)
    packed = grouped[:, :, 0, :] + grouped[:, :, 1, :] * 256 + grouped[:, :, 2, :] * 65536 + top_signed * 16777216
    return packed.astype(jnp.int32)


def plant(entries, rng, low, top_value):
    shape = entries.shape
    place = [jax.random.randint(jax.random.fold_in(rng, axis), (), 0, shape[axis]) for axis in range(len(shape))]
    entries = entries.at[tuple(place)].set(low)
    longest = shape.index(max(shape))
    place[longest] = (place[longest] + 1) % shape[longest]
    return entries.at[tuple(place)].set(top_value)


def shard_levels(stream_key, extent, cuts, smallest, top_value):
    factor_of, own = 1.0, jax.random.fold_in(stream_key, 6)
    for axis_at, parts in cuts:
        heights = jnp.exp(jax.random.uniform(jax.random.fold_in(own, axis_at), (parts,), jnp.float32, smallest / len(cuts), top_value / len(cuts)))
        factor_of = factor_of * jnp.repeat(heights, extent[axis_at] // parts).reshape([-1 if axis == axis_at else 1 for axis in range(len(extent))])
    return factor_of


def setup_inputs(seed: int = 0) -> dict:
    seeds = jax.random.split(jax.random.key(seed), 3)
    probe_bits = plant(jax.random.randint(seeds[0], (NX, NZ // 4, NY), -2147483648, 2147483647), jax.random.fold_in(seeds[0], 1), -2147483648, 2147483646).astype(jnp.int32)
    disorder_levels = draw_disorder_levels(jax.random.fold_in(seeds[2], 71), 0)
    return dict(probe_bits=probe_bits, disorder_levels=disorder_levels)


disorder_width = 4.0
spectral_scale = 8.4


def unpack_signs(packed):
    shifts = 4 * jnp.arange(PROBES, dtype=jnp.int32)[:, None] + jnp.arange(4, dtype=jnp.int32)[None, :]
    bit_values = jnp.right_shift(packed[None, :, :, None, :], shifts[:, None, None, :, None]) & 1
    layout = bit_values.shape
    flat = bit_values.reshape(layout[0], layout[1], layout[2] * layout[3], layout[4])
    return 2.0 * flat.astype(jnp.float32) - 1.0


def unpack_energy(packed):
    shifts = 8 * jnp.arange(4, dtype=jnp.int32)
    levels = jnp.right_shift(packed[:, :, None, :], shifts[None, None, :, None]) & 255
    layout = levels.shape
    flat = levels.reshape(layout[0], layout[1] * layout[2], layout[3])
    return disorder_width * ((flat.astype(jnp.float32) + 0.5) / LEVELS - 0.5)


def apply_ham(field, energy):
    beside = jnp.roll(field, -1, 1) + jnp.roll(field, 1, 1)
    beside = beside + jnp.roll(field, -1, 3) + jnp.roll(field, 1, 3)
    beside = beside + jnp.roll(field, -1, 2) + jnp.roll(field, 1, 2)
    return (energy[None] * field - beside) / spectral_scale


def reference(probe_bits, disorder_levels):
    signs = unpack_signs(probe_bits)
    energy = unpack_energy(disorder_levels)
    first = apply_ham(signs, energy)
    second = 2.0 * apply_ham(first, energy) - signs
    third = 2.0 * apply_ham(second, energy) - first
    moments = jnp.stack([jnp.sum(signs * vec, axis=(1, 2, 3)) for vec in (first, second, third)]) / NSITES
    return moments, second, third
```

```python
import functools

import jax
import jax.numpy as jnp
from jax import lax
from jax.experimental import pallas as pl
from jax.experimental.pallas import tpu as pltpu
from jax.sharding import Mesh
from jax.sharding import PartitionSpec as P

PROBES = 8
LEVELS = 256
NX, NW, NY = 4, 8, 128
NZ = 4 * NW
GY = ("ya", "yb")
GZ = ("za", "zb")
NEAR = ("gx", "ya", "yb", "zb")
FAR = "za"

disorder_width = 4.0
spectral_scale = 8.4
INV = 1.0 / spectral_scale
TWO = 2.0 / spectral_scale
E_MUL = TWO * disorder_width / LEVELS
E_ADD = TWO * disorder_width * (0.5 / LEVELS - 0.5)

PLANES = 18
ROWS = 24


def vmem(n):
    return [pl.BlockSpec(memory_space=pltpu.VMEM)] * n


def lanes(shape):
    return lax.broadcasted_iota(jnp.int32, shape, len(shape) - 1)


def edge_kernel(bits, levels, out):
    lane = lanes((NW, NY))
    word = lax.broadcasted_iota(jnp.int32, (NW, NY), 0)
    mask = (lane // 16 == word) & (lane % 16 < 6)
    for a, src in enumerate((bits, levels)):
        for x in range(NX):
            rolled = pltpu.roll(src[x], 3, 1, stride=16, stride_axis=0)
            out[a * NX + x : a * NX + x + 1] = jnp.sum(
                jnp.where(mask, rolled, 0), axis=0, keepdims=True
            )


def face_kernel(where, bits, levels, left, right, edges, low, high):
    del where
    lane = lanes((NW, NY))
    both = jnp.where(lane % 16 < 3, left[...], right[...])
    edges[...] = both
    for out, first in ((low, 0), (high, 1)):
        for i in range(3):
            out[8 * i : 8 * i + 8] = bits[first + i]
        for i in range(2):
            out[24 + 8 * i : 32 + 8 * i] = levels[2 * first + i]
        out[40:48] = both


def plane_list(bits, levels, edges, below, above):
    found = []
    for x in range(-3, 7):
        if x < 0:
            found.append((below, 8 * (x + 3), below, 40 + x + 4))
        elif x < NX:
            found.append((bits, x, edges, x))
        else:
            found.append((above, 8 * (x - 4), above, 40 + x - 4))
    for x in range(-2, 6):
        if x < 0:
            found.append((below, 24 + 8 * (x + 2), below, 44 + x + 4))
        elif x < NX:
            found.append((levels, x, edges, 4 + x))
        else:
            found.append((above, 24 + 8 * (x - 4), above, 44 + x - 4))
    return found


def word_row(plane, w):
    ref, at = plane[:2]
    if len(ref.shape) == 3:
        return ref[at, w : w + 1, :]
    return ref[at + w : at + w + 1, :]


def shift_edges(rows, w):
    return pltpu.roll(rows, (-(16 * w + 3)) % NY, 1)


def level_kernel(bits, levels, edges, below, above, low, high, strip):
    planes = plane_list(bits, levels, edges, below, above)
    strip[PLANES - PLANES % 8 :] = jnp.zeros((8, NY), jnp.int32)
    for k, plane in enumerate(planes):
        strip[k : k + 1] = plane[2][plane[3] : plane[3] + 1, :]
    for out, w in ((low, 0), (high, NW - 1)):
        out[16:24] = jnp.zeros((8, NY), jnp.int32)
        for k, plane in enumerate(planes):
            out[k : k + 1] = word_row(plane, w)
        out[ROWS:] = shift_edges(strip[...], w)


def field_kernel(
    bits, levels, edges, below, above, under, over,
    previous, current, message,
    strip, borders, v0, energy, v1, v2,
):
    planes = plane_list(bits, levels, edges, below, above)
    strip[16:24] = jnp.zeros((8, NY), jnp.int32)
    for k, plane in enumerate(planes):
        strip[k : k + 1] = plane[2][plane[3] : plane[3] + 1, :]
    for w in range(NW):
        borders[w] = shift_edges(strip[...], w)

    tile = (PROBES, NY)
    probe = lax.broadcasted_iota(jnp.int32, tile, 0)
    lane = lanes(tile)
    bit_of = [jnp.left_shift(1, 4 * probe + j) for j in range(4)]
    first_lane, last_lane = lane == 0, lane == NY - 1

    def rows_of(k, w):
        if w < 0:
            pair = under[k : k + 1, :], under[ROWS + k : ROWS + k + 1, :]
        elif w >= NW:
            pair = over[k : k + 1, :], over[ROWS + k : ROWS + k + 1, :]
        else:
            pair = word_row(planes[k], w), borders[w, k : k + 1, :]
        return [jnp.broadcast_to(row, tile) for row in pair]

    for k in range(10):
        for w in range(-1, NW + 1):
            for half, row in enumerate(rows_of(k, w)):
                for j in range(4):
                    z = 4 * w + j
                    if -3 <= z < NZ + 3:
                        v0[k, z + 3, :, NY * half : NY * (half + 1)] = jnp.where(
                            (row & bit_of[j]) != 0, 1.0, -1.0
                        )
    for k in range(8):
        for w in range(-1, NW + 1):
            for half, row in enumerate(rows_of(10 + k, w)):
                for j in range(4):
                    z = 4 * w + j
                    if -2 <= z < NZ + 2:
                        level = jnp.right_shift(row, 8 * j) & 255
                        energy[k, z + 2, :, NY * half : NY * (half + 1)] = (
                            level.astype(jnp.float32) * E_MUL + E_ADD
                        )

    def get(ref, x, z):
        return ref[x, z, :, :NY], ref[x, z, :, NY:]

    def step(ref, x, z, ex, ez, main_only=False):
        m, e = get(ref, x, z)
        up_m, up_e = pltpu.roll(m, NY - 1, 1), pltpu.roll(e, NY - 1, 1)
        dn_m, dn_e = pltpu.roll(m, 1, 1), pltpu.roll(e, 1, 1)
        beside = [jnp.where(last_lane, up_e, up_m) + jnp.where(first_lane, dn_e, dn_m)]
        if not main_only:
            beside.append(jnp.where(last_lane, up_m, up_e) + jnp.where(first_lane, dn_m, dn_e))
        result = []
        for half, s in enumerate(beside):
            at = slice(NY * half, NY * (half + 1))
            s = s + (ref[x + 1, z, :, at] + ref[x - 1, z, :, at])
            s = s + (ref[x, z + 1, :, at] + ref[x, z - 1, :, at])
            result.append(energy[ex, ez, :, at] * (m, e)[half] - TWO * s)
        return result

    UNROLL = 4
    for x in range(8):

        def first(i, carry, x=x):
            for u in range(UNROLL):
                z = i * UNROLL + u
                for half, t in enumerate(step(v0, x + 1, z + 1, x, z)):
                    v1[x, z, :, NY * half : NY * (half + 1)] = 0.5 * t
            return carry

        lax.fori_loop(0, (NZ + 4) // UNROLL, first, 0)

    for x in range(6):

        def second(i, carry, x=x):
            for u in range(2):
                z = i * 2 + u
                for half, t in enumerate(step(v1, x + 1, z + 1, x + 1, z + 1)):
                    at = slice(NY * half, NY * (half + 1))
                    v2[x, z, :, at] = t - v0[x + 2, z + 2, :, at]
            return carry

        lax.fori_loop(0, (NZ + 2) // 2, second, 0)

    sums = [jnp.zeros(tile, jnp.float32)] * 3
    for x in range(NX):

        def third(i, sums, x=x):
            sums = list(sums)
            for u in range(UNROLL):
                z = i * UNROLL + u
                t = step(v2, x + 1, z + 1, x + 2, z + 2, main_only=True)[0]
                one = v1[x + 2, z + 2, :, :NY]
                two = v2[x + 1, z + 1, :, :NY]
                three = t - one
                previous[pl.ds(x * NZ + z, PROBES, stride=NX * NZ), :] = two
                current[pl.ds(x * NZ + z, PROBES, stride=NX * NZ), :] = three
                sign = v0[x + 3, z + 3, :, :NY]
                sums = [acc + sign * v for acc, v in zip(sums, (one, two, three))]
            return tuple(sums)

        sums = lax.fori_loop(0, NZ // UNROLL, third, tuple(sums))

    row = jnp.zeros(tile, jnp.float32)
    for n, acc in enumerate(sums):
        total = jnp.sum(acc, axis=1, keepdims=True)
        row = jnp.where(lane == 8 * n + probe, total, row)
    row = jnp.sum(row, axis=0, keepdims=True)
    message[...] = jnp.broadcast_to(row, message.shape)


def shape(rows, dtype=jnp.int32):
    return jax.ShapeDtypeStruct(rows, dtype)


def shift(array, axis, by):
    count = lax.axis_size(axis)
    return lax.ppermute(array, axis, [(i, (i + by) % count) for i in range(count)])


def per_device(bits, levels):
    tile = (NW, NY)
    edge = pl.pallas_call(
        edge_kernel, out_shape=shape(tile), in_specs=vmem(2), out_specs=vmem(1)[0], name="edge"
    )(bits, levels)
    gathered = lax.all_gather(edge, GY)
    count = lax.axis_size(GY)
    here = lax.axis_index(GY)
    where = jnp.stack([(here + count - 1) % count, (here + 1) % count]).astype(jnp.int32)
    whole = pl.BlockSpec((NX, NW, NY), lambda i, w: (0, 0, 0))
    flat = lambda rows: pl.BlockSpec((rows, NY), lambda i, w: (0, 0))
    edges, low, high = pl.pallas_call(
        face_kernel,
        out_shape=(shape(tile), shape((48, NY)), shape((48, NY))),
        grid_spec=pltpu.PrefetchScalarGridSpec(
            num_scalar_prefetch=1,
            grid=(1,),
            in_specs=[
                whole,
                whole,
                pl.BlockSpec((None, NW, NY), lambda i, w: (w[0], 0, 0)),
                pl.BlockSpec((None, NW, NY), lambda i, w: (w[1], 0, 0)),
            ],
            out_specs=[flat(NW), flat(48), flat(48)],
        ),
        name="face",
    )(where, bits, levels, gathered, gathered)
    below = shift(high, "gx", 1)
    above = shift(low, "gx", -1)
    z_low, z_high = pl.pallas_call(
        level_kernel,
        out_shape=(shape((2 * ROWS, NY)),) * 2,
        in_specs=vmem(5),
        out_specs=tuple(vmem(2)),
        scratch_shapes=[pltpu.VMEM((ROWS, NY), jnp.int32)],
        name="level",
    )(bits, levels, edges, below, above)
    under = shift(z_high, GZ, 1)
    over = shift(z_low, GZ, -1)
    near = 1
    for axis in NEAR:
        near *= lax.axis_size(axis)
    far = lax.axis_size(FAR)
    total = near * far * NX * NZ * NY
    f32 = jnp.float32
    previous, current, message = pl.pallas_call(
        field_kernel,
        out_shape=(
            shape((PROBES * NX * NZ, NY), f32),
            shape((PROBES * NX * NZ, NY), f32),
            shape((near, NY), f32),
        ),
        in_specs=vmem(7),
        out_specs=tuple(vmem(3)),
        scratch_shapes=[
            pltpu.VMEM((ROWS, NY), jnp.int32),
            pltpu.VMEM((NW, ROWS, NY), jnp.int32),
            pltpu.VMEM((NX + 6, NZ + 6, PROBES, 2 * NY), f32),
            pltpu.VMEM((NX + 4, NZ + 4, PROBES, 2 * NY), f32),
            pltpu.VMEM((NX + 4, NZ + 4, PROBES, 2 * NY), f32),
            pltpu.VMEM((NX + 2, NZ + 2, PROBES, 2 * NY), f32),
        ],
        name="field",
    )(bits, levels, edges, below, above, under, over)
    part = jnp.sum(lax.all_to_all(message, NEAR, 0, 0, tiled=True), axis=0, keepdims=True)
    spread = jnp.broadcast_to(part, (far, NY))
    summed = jnp.sum(lax.all_to_all(spread, FAR, 0, 0, tiled=True), axis=0)
    moments = summed[: 3 * PROBES].reshape(3, PROBES) / total
    block = (PROBES, NX, NZ, NY)
    return moments, previous.reshape(block), current.reshape(block)


def solution(mesh):
    sizes = mesh.shape["gx"], mesh.shape["gy"], mesh.shape["gz"]
    torus = Mesh(
        mesh.devices.reshape(sizes[0], sizes[1] // 2, 2, sizes[2] // 2, 2),
        ("gx",) + GY + GZ,
    )
    return jax.shard_map(
        per_device,
        mesh=torus,
        in_specs=(P("gx", GZ, GY), P("gx", GZ, GY)),
        out_specs=(P(), P(None, "gx", GZ, GY), P(None, "gx", GZ, GY)),
        check_vma=False,
    )
```

```python
import functools

import jax
import jax.numpy as jnp
from jax import lax
from jax.experimental import pallas as pl
from jax.experimental.pallas import tpu as pltpu
from jax.sharding import Mesh
from jax.sharding import PartitionSpec as P

PROBES = 8
LEVELS = 256
NX, NW, NY = 4, 8, 128
NZ = 4 * NW
PITCH = NZ + 8
GY = ("ya", "yb")
GZ = ("za", "zb")
NEAR = ("gx", "ya", "yb", "zb")
FAR = "za"

disorder_width = 4.0
spectral_scale = 8.4
INV = 1.0 / spectral_scale
TWO = 2.0 / spectral_scale
E_MUL = TWO * disorder_width / LEVELS
E_ADD = TWO * disorder_width * (0.5 / LEVELS - 0.5)

PLANES = 18
ROWS = 24


def vmem(n):
    return [pl.BlockSpec(memory_space=pltpu.VMEM)] * n


def lanes(shape):
    return lax.broadcasted_iota(jnp.int32, shape, len(shape) - 1)


def edge_kernel(bits, levels, out, bits_kept, levels_kept):
    bits_kept[...] = bits[...]
    levels_kept[...] = levels[...]
    lane = lanes((NW, NY))
    word = lax.broadcasted_iota(jnp.int32, (NW, NY), 0)
    mask = (lane // 16 == word) & (lane % 16 < 6)
    for a, src in enumerate((bits, levels)):
        for x in range(NX):
            rolled = pltpu.roll(src[x], 3, 1, stride=16, stride_axis=0)
            out[a * NX + x : a * NX + x + 1] = jnp.sum(
                jnp.where(mask, rolled, 0), axis=0, keepdims=True
            )


def face_kernel(bits, levels, gathered, edges, low, high):
    count = gathered.shape[0] // NW
    here = 2 * lax.axis_index("ya") + lax.axis_index("yb")
    left = gathered[pl.ds(NW * ((here + count - 1) % count), NW), :]
    right = gathered[pl.ds(NW * ((here + 1) % count), NW), :]
    lane = lanes((NW, NY))
    both = jnp.where(lane % 16 < 3, left, right)
    edges[...] = both
    for out, first in ((low, 0), (high, 1)):
        for i in range(3):
            out[8 * i : 8 * i + 8] = bits[first + i]
        for i in range(2):
            out[24 + 8 * i : 32 + 8 * i] = levels[2 * first + i]
        out[40:48] = both


def plane_list(bits, levels, edges, below, above):
    found = []
    for x in range(-3, 7):
        if x < 0:
            found.append((below, 8 * (x + 3), below, 40 + x + 4))
        elif x < NX:
            found.append((bits, x, edges, x))
        else:
            found.append((above, 8 * (x - 4), above, 40 + x - 4))
    for x in range(-2, 6):
        if x < 0:
            found.append((below, 24 + 8 * (x + 2), below, 44 + x + 4))
        elif x < NX:
            found.append((levels, x, edges, 4 + x))
        else:
            found.append((above, 24 + 8 * (x - 4), above, 44 + x - 4))
    return found


def word_row(plane, w):
    ref, at = plane[:2]
    if len(ref.shape) == 3:
        return ref[at, w : w + 1, :]
    return ref[at + w : at + w + 1, :]


def shift_edges(rows, w):
    return pltpu.roll(rows, (-(16 * w + 3)) % NY, 1)


def level_kernel(bits, levels, edges, below, above, low, high, strip):
    planes = plane_list(bits, levels, edges, below, above)
    strip[PLANES - PLANES % 8 :] = jnp.zeros((8, NY), jnp.int32)
    for k, plane in enumerate(planes):
        strip[k : k + 1] = plane[2][plane[3] : plane[3] + 1, :]
    for out, w in ((low, 0), (high, NW - 1)):
        out[16:24] = jnp.zeros((8, NY), jnp.int32)
        for k, plane in enumerate(planes):
            out[k : k + 1] = word_row(plane, w)
        out[ROWS:] = shift_edges(strip[...], w)


def field_kernel(
    bits, levels, edges, below, above, under, over,
    previous, current, message,
    strip, borders, v0, energy, v1, v2, blocks, done,
):
    planes = plane_list(bits, levels, edges, below, above)
    strip[16:24] = jnp.zeros((8, NY), jnp.int32)
    for k, plane in enumerate(planes):
        strip[k : k + 1] = plane[2][plane[3] : plane[3] + 1, :]
    for w in range(NW):
        borders[w] = shift_edges(strip[...], w)

    tile = (PROBES, NY)
    probe = lax.broadcasted_iota(jnp.int32, tile, 0)
    lane = lanes(tile)
    bit_of = [jnp.left_shift(1, 4 * probe + j) for j in range(4)]
    first_lane, last_lane = lane == 0, lane == NY - 1

    def rows_of(k, w):
        if w < 0:
            pair = under[k : k + 1, :], under[ROWS + k : ROWS + k + 1, :]
        elif w >= NW:
            pair = over[k : k + 1, :], over[ROWS + k : ROWS + k + 1, :]
        else:
            pair = word_row(planes[k], w), borders[w, k : k + 1, :]
        return [jnp.broadcast_to(row, tile) for row in pair]

    for k in range(10):
        for w in range(-1, NW + 1):
            for half, row in enumerate(rows_of(k, w)):
                for j in range(4):
                    z = 4 * w + j
                    if -3 <= z < NZ + 3:
                        v0[k, z + 3, :, NY * half : NY * (half + 1)] = jnp.where(
                            (row & bit_of[j]) != 0, 1.0, -1.0
                        )
    for k in range(8):
        for w in range(-1, NW + 1):
            for half, row in enumerate(rows_of(10 + k, w)):
                for j in range(4):
                    z = 4 * w + j
                    if -2 <= z < NZ + 2:
                        level = jnp.right_shift(row, 8 * j) & 255
                        energy[k, z + 2, :, NY * half : NY * (half + 1)] = (
                            level.astype(jnp.float32) * E_MUL + E_ADD
                        )

    def get(ref, x, z):
        return ref[x, z, :, :NY], ref[x, z, :, NY:]

    def step(ref, x, z, ex, ez, main_only=False):
        m, e = get(ref, x, z)
        up_m, up_e = pltpu.roll(m, NY - 1, 1), pltpu.roll(e, NY - 1, 1)
        dn_m, dn_e = pltpu.roll(m, 1, 1), pltpu.roll(e, 1, 1)
        beside = [jnp.where(last_lane, up_e, up_m) + jnp.where(first_lane, dn_e, dn_m)]
        if not main_only:
            beside.append(jnp.where(last_lane, up_m, up_e) + jnp.where(first_lane, dn_m, dn_e))
        result = []
        for half, s in enumerate(beside):
            at = slice(NY * half, NY * (half + 1))
            s = s + (ref[x + 1, z, :, at] + ref[x - 1, z, :, at])
            s = s + (ref[x, z + 1, :, at] + ref[x, z - 1, :, at])
            result.append(energy[ex, ez, :, at] * (m, e)[half] - TWO * s)
        return result

    def first(x, carry):
        for z in range(NZ + 4):
            for half, t in enumerate(step(v0, x + 1, z + 1, x, z)):
                v1[x, z, :, NY * half : NY * (half + 1)] = 0.5 * t
        return carry

    lax.fori_loop(0, NX + 4, first, 0)

    def second(x, carry):
        for z in range(NZ + 2):
            for half, t in enumerate(step(v1, x + 1, z + 1, x + 1, z + 1)):
                at = slice(NY * half, NY * (half + 1))
                v2[x, z, :, at] = t - v0[x + 2, z + 2, :, at]
        return carry

    lax.fori_loop(0, NX + 2, second, 0)

    rows = blocks.reshape(2 * NX * PROBES * PITCH, NY)

    def copy_out(n, x):
        return pltpu.make_async_copy(
            blocks.at[n, x, :, pl.ds(0, NZ), :], (previous, current)[n].at[:, x], done.at[n, x]
        )

    def third(x, sums):
        sums = list(sums)
        for z in range(NZ):
            t = step(v2, x + 1, z + 1, x + 2, z + 2, main_only=True)[0]
            one = v1[x + 2, z + 2, :, :NY]
            two = v2[x + 1, z + 1, :, :NY]
            three = t - one
            for n, v in enumerate((two, three)):
                at = (n * NX + x) * PROBES * PITCH + z
                rows[pl.ds(at, PROBES, stride=PITCH), :] = v
            sign = v0[x + 3, z + 3, :, :NY]
            sums = [acc + sign * v for acc, v in zip(sums, (one, two, three))]
        copy_out(0, x).start()
        copy_out(1, x).start()
        return tuple(sums)

    sums = lax.fori_loop(0, NX, third, (jnp.zeros(tile, jnp.float32),) * 3)

    row = jnp.zeros(tile, jnp.float32)
    for n, acc in enumerate(sums):
        total = jnp.sum(acc, axis=1, keepdims=True)
        row = jnp.where(lane == 8 * n + probe, total, row)
    row = jnp.sum(row, axis=0, keepdims=True)
    message[...] = jnp.broadcast_to(row, message.shape)
    for n in range(2):
        for x in range(NX):
            copy_out(n, x).wait()


def local(rows, dtype=jnp.int32):
    return pltpu.VMEM(rows, dtype)


def keep(array):
    return pltpu.with_memory_space_constraint(array, pltpu.VMEM)


def shift(array, axis, by):
    count = lax.axis_size(axis)
    return lax.ppermute(array, axis, [(i, (i + by) % count) for i in range(count)])


def per_device(bits, levels):
    tile = (NW, NY)
    edge, bits, levels = pl.pallas_call(
        edge_kernel,
        out_shape=(local(tile), local(bits.shape), local(levels.shape)),
        in_specs=vmem(2),
        out_specs=tuple(vmem(3)),
        name="edge",
    )(bits, levels)
    bits, levels = keep(bits), keep(levels)
    gathered = keep(lax.all_gather(edge, GY, tiled=True))
    edges, low, high = pl.pallas_call(
        face_kernel,
        out_shape=(local(tile), local((48, NY)), local((48, NY))),
        in_specs=vmem(3),
        out_specs=tuple(vmem(3)),
        name="face",
    )(bits, levels, gathered)
    edges = keep(edges)
    below = keep(shift(high, "gx", 1))
    above = keep(shift(low, "gx", -1))
    z_low, z_high = pl.pallas_call(
        level_kernel,
        out_shape=(local((2 * ROWS, NY)),) * 2,
        in_specs=vmem(5),
        out_specs=tuple(vmem(2)),
        scratch_shapes=[pltpu.VMEM((ROWS, NY), jnp.int32)],
        name="level",
    )(bits, levels, edges, below, above)
    under = keep(shift(z_high, GZ, 1))
    over = keep(shift(z_low, GZ, -1))
    near = 1
    for axis in NEAR:
        near *= lax.axis_size(axis)
    far = lax.axis_size(FAR)
    total = near * far * NX * NZ * NY
    f32 = jnp.float32
    block = (PROBES, NX, NZ, NY)
    hbm = pl.BlockSpec(memory_space=pl.ANY)
    previous, current, message = pl.pallas_call(
        field_kernel,
        out_shape=(
            jax.ShapeDtypeStruct(block, f32),
            jax.ShapeDtypeStruct(block, f32),
            local((near, NY), f32),
        ),
        in_specs=vmem(7),
        out_specs=(hbm, hbm, vmem(1)[0]),
        scratch_shapes=[
            pltpu.VMEM((ROWS, NY), jnp.int32),
            pltpu.VMEM((NW, ROWS, NY), jnp.int32),
            pltpu.VMEM((NX + 6, NZ + 6, PROBES, 2 * NY), f32),
            pltpu.VMEM((NX + 4, NZ + 4, PROBES, 2 * NY), f32),
            pltpu.VMEM((NX + 4, NZ + 4, PROBES, 2 * NY), f32),
            pltpu.VMEM((NX + 2, NZ + 2, PROBES, 2 * NY), f32),
            pltpu.VMEM((2, NX, PROBES, PITCH, NY), f32),
            pltpu.SemaphoreType.DMA((2, NX)),
        ],
        name="field",
    )(bits, levels, edges, below, above, under, over)
    part = jnp.sum(lax.all_to_all(message, NEAR, 0, 0, tiled=True), axis=0, keepdims=True)
    spread = jnp.broadcast_to(part, (far, NY))
    summed = jnp.sum(lax.all_to_all(spread, FAR, 0, 0, tiled=True), axis=0)
    moments = summed[: 3 * PROBES].reshape(3, PROBES) / total
    return moments, previous, current


def solution(mesh):
    sizes = mesh.shape["gx"], mesh.shape["gy"], mesh.shape["gz"]
    torus = Mesh(
        mesh.devices.reshape(sizes[0], sizes[1] // 2, 2, sizes[2] // 2, 2),
        ("gx",) + GY + GZ,
    )
    return jax.shard_map(
        per_device,
        mesh=torus,
        in_specs=(P("gx", GZ, GY), P("gx", GZ, GY)),
        out_specs=(P(), P(None, "gx", GZ, GY), P(None, "gx", GZ, GY)),
        check_vma=False,
    )
```

```python
import jax
import jax.numpy as jnp
from jax import lax
from jax.experimental import pallas as pl
from jax.experimental.pallas import tpu as pltpu
from jax.sharding import Mesh
from jax.sharding import PartitionSpec as P

PROBES = 8
LEVELS = 256
NX, NW, NY = 4, 8, 128
NZ = 4 * NW
PITCH = NZ + 8
GY = ("ya", "yb")
GZ = ("za", "zb")
REST = ("gx",) + GZ

disorder_width = 4.0
spectral_scale = 8.4
TWO = 2.0 / spectral_scale
E_MUL = TWO * disorder_width / LEVELS
E_ADD = TWO * disorder_width * (0.5 / LEVELS - 0.5)

PLANES = 18
ROWS = 24
FRACTION = 2.0**20


def vmem(n):
    return [pl.BlockSpec(memory_space=pltpu.VMEM)] * n


def lanes(shape):
    return lax.broadcasted_iota(jnp.int32, shape, len(shape) - 1)


def face_kernel(bits, levels, low, high, bits_kept, levels_kept):
    bits_kept[...] = bits[...]
    levels_kept[...] = levels[...]
    for out, first in ((low, 0), (high, 1)):
        for i in range(3):
            out[8 * i : 8 * i + 8] = bits[first + i]
        for i in range(2):
            out[24 + 8 * i : 32 + 8 * i] = levels[2 * first + i]


def plane_list(bits, levels, below, above):
    found = []
    for x in range(-3, 7):
        if x < 0:
            found.append((below, 8 * (x + 3)))
        elif x < NX:
            found.append((bits, x))
        else:
            found.append((above, 8 * (x - 4)))
    for x in range(-2, 6):
        if x < 0:
            found.append((below, 24 + 8 * (x + 2)))
        elif x < NX:
            found.append((levels, x))
        else:
            found.append((above, 24 + 8 * (x - 4)))
    return found


def plane_tile(plane):
    ref, at = plane
    if len(ref.shape) == 3:
        return ref[at]
    return ref[at : at + NW, :]


def word_row(plane, w):
    ref, at = plane
    if len(ref.shape) == 3:
        return ref[at, w : w + 1, :]
    return ref[at + w : at + w + 1, :]


def level_kernel(bits, levels, below, above, low, high):
    planes = plane_list(bits, levels, below, above)
    for out, w in ((low, 0), (high, NW - 1)):
        out[16:24] = jnp.zeros((8, NY), jnp.int32)
        for k, plane in enumerate(planes):
            out[k : k + 1] = word_row(plane, w)


def tiles():
    tile = (PROBES, NY)
    probe = lax.broadcasted_iota(jnp.int32, tile, 0)
    return tile, probe, lanes(tile), [jnp.left_shift(1, 4 * probe + j) for j in range(4)]


def sign_of(row, bit):
    return jnp.where((row & bit) != 0, 1.0, -1.0)


def energy_of(row, j):
    return (jnp.right_shift(row, 8 * j) & 255).astype(jnp.float32) * E_MUL + E_ADD


def step(v, energy, at, place):
    x, z = at
    own = v[x, z]
    s = pltpu.roll(own, NY - 1, 1) + pltpu.roll(own, 1, 1)
    s = s + (v[x + 1, z] + v[x - 1, z])
    s = s + (v[x, z + 1] + v[x, z - 1])
    return energy[place] * own - TWO * s


def sums_row(sums, mask, probe, lane):
    row = jnp.zeros(lane.shape, jnp.float32)
    for n, acc in enumerate(sums):
        total = jnp.sum(jnp.where(mask, acc, 0.0), axis=1, keepdims=True)
        row = jnp.where(lane == 8 * n + probe, total, row)
    return jnp.sum(row, axis=0, keepdims=True)


def main_kernel(
    bits, levels, below, above, under, over,
    strips, v2, v3,
    v0, energy, v1,
):
    planes = plane_list(bits, levels, below, above)
    tile, probe, lane, bit_of = tiles()

    word = lax.broadcasted_iota(jnp.int32, tile, 0)
    mask = (lane // 16 == word) & (lane % 16 < 12)
    strips[16:24] = jnp.zeros((8, NY), jnp.int32)
    for k, plane in enumerate(planes):
        rolled = pltpu.roll(plane_tile(plane), 6, 1, stride=16, stride_axis=0)
        strips[k : k + 1] = jnp.sum(jnp.where(mask, rolled, 0), axis=0, keepdims=True)
    wide = lanes((ROWS, NY))
    strips[ROWS:] = jnp.where(
        wide < 16, pltpu.roll(under[...], 6, 1), pltpu.roll(over[...], 6 + 112, 1)
    )

    def row_of(k, w):
        if w < 0:
            row = under[k : k + 1, :]
        elif w >= NW:
            row = over[k : k + 1, :]
        else:
            row = word_row(planes[k], w)
        return jnp.broadcast_to(row, tile)

    for w in range(-1, NW + 1):
        for k in range(10):
            row = row_of(k, w)
            for j in range(4):
                z = 4 * w + j
                if -3 <= z < NZ + 3:
                    v0[k, z + 3] = sign_of(row, bit_of[j])
        for k in range(8):
            row = row_of(10 + k, w)
            for j in range(4):
                z = 4 * w + j
                if -2 <= z < NZ + 2:
                    energy[k, z + 2] = energy_of(row, j)

    def first(i, carry):
        for u in range(2):
            x = 2 * i + u
            for z in range(NZ + 4):
                v1[x, z] = 0.5 * step(v0, energy, (x + 1, z + 1), (x, z))
        return carry

    lax.fori_loop(0, (NX + 4) // 2, first, 0)

    def second(i, carry):
        for u in range(2):
            x = 2 * i + u
            for z in range(NZ + 2):
                v2[x, z] = step(v1, energy, (x + 1, z + 1), (x + 1, z + 1)) - v0[x + 2, z + 2]
        return carry

    lax.fori_loop(0, (NX + 2) // 2, second, 0)

    def third(i, sums):
        sums = list(sums)
        for u in range(2):
            x = 2 * i + u
            for z in range(NZ):
                one = v1[x + 2, z + 2]
                two = v2[x + 1, z + 1]
                three = step(v2, energy, (x + 1, z + 1), (x + 2, z + 2)) - one
                v3[x, z] = three
                sign = v0[x + 3, z + 3]
                sums = [acc + sign * v for acc, v in zip(sums, (one, two, three))]
        return tuple(sums)

    sums = lax.fori_loop(0, NX // 2, third, (jnp.zeros(tile, jnp.float32),) * 3)
    row = sums_row(sums, (lane >= 3) & (lane < NY - 3), probe, lane)
    whole = row.astype(jnp.int32)
    part = (row - whole.astype(jnp.float32)) * FRACTION
    strips[PLANES : PLANES + 1] = whole
    strips[PLANES + 1 : PLANES + 2] = part.astype(jnp.int32)


def edge_kernel(
    gathered, v2, v3,
    previous, current, message,
    words, e0, energy, e1, e2, e3, blocks, done,
):
    count = gathered.shape[0] // (2 * ROWS)
    tile, probe, lane, bit_of = tiles()
    wide = lanes((ROWS, NY))

    def interfaces(i, sums):
        sums = list(sums)
        for u in range(2):
            k = 2 * i + u
            here, there = 2 * ROWS * k, 2 * ROWS * ((k + 1) % count)
            left = wide % 16 < 6
            own = jnp.where(left, gathered[pl.ds(here, ROWS), :], gathered[pl.ds(there, ROWS), :])
            far = jnp.where(
                left,
                gathered[pl.ds(here + ROWS, ROWS), :],
                gathered[pl.ds(there + ROWS, ROWS), :],
            )
            words[u, 0] = jnp.where(wide < 16, far, pltpu.roll(own, 16, 1))
            words[u, 1] = own
            words[u, 2] = jnp.where(wide >= 112, far, pltpu.roll(own, 112, 1))
        for u in range(2):
            for n in range(3):
                for k in range(10):
                    row = jnp.broadcast_to(words[u, n, k : k + 1, :], tile)
                    for j in range(4):
                        z = 4 * n - 4 + j
                        if -3 <= z < 7:
                            e0[u, k, z + 3] = sign_of(row, bit_of[j])
                for k in range(8):
                    row = jnp.broadcast_to(words[u, n, 10 + k : 11 + k, :], tile)
                    for j in range(4):
                        z = 4 * n - 4 + j
                        if -2 <= z < 6:
                            energy[u, k, z + 2] = energy_of(row, j)
        for u in range(2):
            for x in range(8):
                for z in range(8):
                    e1[u, x, z] = 0.5 * step(e0.at[u], energy.at[u], (x + 1, z + 1), (x, z))
        for u in range(2):
            for x in range(6):
                for z in range(6):
                    e2[2 * i + u, x, z] = (
                        step(e1.at[u], energy.at[u], (x + 1, z + 1), (x + 1, z + 1))
                        - e0[u, x + 2, z + 2]
                    )
        for u in range(2):
            for x in range(4):
                for z in range(4):
                    one = e1[u, x + 2, z + 2]
                    two = e2[2 * i + u, x + 1, z + 1]
                    three = (
                        step(e2.at[2 * i + u], energy.at[u], (x + 1, z + 1), (x + 2, z + 2)) - one
                    )
                    e3[2 * i + u, x, z] = three
                    sign = e0[u, x + 3, z + 3]
                    sums = [acc + sign * v for acc, v in zip(sums, (one, two, three))]
        return tuple(sums)

    sums = lax.fori_loop(0, count // 2, interfaces, (jnp.zeros(tile, jnp.float32),) * 3)

    here = 2 * lax.axis_index("ya") + lax.axis_index("yb")
    before = (here + count - 1) % count
    right = lane % 16 < 6
    outside = (lane < 3) | (lane >= NY - 3)
    rows = blocks.reshape(2 * NX * PROBES * PITCH, NY)

    def copy_out(n, x):
        return pltpu.make_async_copy(
            blocks.at[n, x, :, pl.ds(0, NZ), :], (previous, current)[n].at[:, x], done.at[n, x]
        )

    def merge(x, carry):
        for n, (main, edge, margin) in enumerate(((v2, e2, 1), (v3, e3, 0))):
            for j in range(4):
                fix = jnp.where(
                    right,
                    edge[here, x + margin, j + margin],
                    edge[before, x + margin, j + margin],
                )
                for w in range(NW):
                    z = 4 * w + j
                    moved = pltpu.roll(fix, (-16 * w - 6) % NY, 1)
                    value = jnp.where(outside, moved, main[x + margin, z + margin])
                    at = (n * NX + x) * PROBES * PITCH + z
                    rows[pl.ds(at, PROBES, stride=PITCH), :] = value
            copy_out(n, x).start()
        return carry

    lax.fori_loop(0, NX, merge, 0)

    row = sums_row(sums, (lane % 16 >= 3) & (lane % 16 < 9), probe, lane)
    for k in range(count):
        at = 2 * ROWS * k + PLANES
        whole = gathered[at : at + 1, :].astype(jnp.float32)
        part = gathered[at + 1 : at + 2, :].astype(jnp.float32)
        row = row + (whole + part * (1.0 / FRACTION))
    message[...] = jnp.broadcast_to(row, message.shape)
    for n in range(2):
        for x in range(NX):
            copy_out(n, x).wait()


def local(rows, dtype=jnp.int32):
    return pltpu.VMEM(rows, dtype)


def keep(array):
    return pltpu.with_memory_space_constraint(array, pltpu.VMEM)


def shift(array, axis, by):
    count = lax.axis_size(axis)
    return lax.ppermute(array, axis, [(i, (i + by) % count) for i in range(count)])


def per_device(bits, levels):
    f32 = jnp.float32
    low, high, bits, levels = pl.pallas_call(
        face_kernel,
        out_shape=(local((40, NY)), local((40, NY)), local(bits.shape), local(levels.shape)),
        in_specs=vmem(2),
        out_specs=tuple(vmem(4)),
        name="face",
    )(bits, levels)
    bits, levels = keep(bits), keep(levels)
    below = keep(shift(high, "gx", 1))
    above = keep(shift(low, "gx", -1))
    z_low, z_high = pl.pallas_call(
        level_kernel,
        out_shape=(local((ROWS, NY)),) * 2,
        in_specs=vmem(4),
        out_specs=tuple(vmem(2)),
        name="level",
    )(bits, levels, below, above)
    under = keep(shift(z_high, GZ, 1))
    over = keep(shift(z_low, GZ, -1))

    def field(margin, z_margin):
        return (NX + 2 * margin, NZ + 2 * z_margin, PROBES, NY)

    strips, v2, v3 = pl.pallas_call(
        main_kernel,
        out_shape=(
            local((2 * ROWS, NY)),
            local(field(1, 1), f32),
            local(field(0, 0), f32),
        ),
        in_specs=vmem(6),
        out_specs=tuple(vmem(3)),
        scratch_shapes=[
            pltpu.VMEM(field(3, 3), f32),
            pltpu.VMEM(field(2, 2), f32),
            pltpu.VMEM(field(2, 2), f32),
        ],
        name="main",
    )(bits, levels, below, above, under, over)
    gathered = keep(lax.all_gather(strips, GY, tiled=True))
    count = lax.axis_size(GY)
    rest = lax.axis_size(REST)
    total = rest * count * NX * NZ * NY
    block = (PROBES, NX, NZ, NY)
    hbm = pl.BlockSpec(memory_space=pl.ANY)

    def edge(n, margin):
        return pltpu.VMEM((n, 4 + 2 * margin, 4 + 2 * margin, PROBES, NY), f32)

    previous, current, message = pl.pallas_call(
        edge_kernel,
        out_shape=(
            jax.ShapeDtypeStruct(block, f32),
            jax.ShapeDtypeStruct(block, f32),
            local((rest, NY), f32),
        ),
        in_specs=vmem(3),
        out_specs=(hbm, hbm, vmem(1)[0]),
        scratch_shapes=[
            pltpu.VMEM((2, 3, ROWS, NY), jnp.int32),
            edge(2, 3),
            edge(2, 2),
            edge(2, 2),
            edge(count, 1),
            edge(count, 0),
            pltpu.VMEM((2, NX, PROBES, PITCH, NY), f32),
            pltpu.SemaphoreType.DMA((2, NX)),
        ],
        name="edges",
    )(gathered, keep(v2), keep(v3))
    summed = jnp.sum(lax.all_to_all(message, REST, 0, 0, tiled=True), axis=0)
    moments = summed[: 3 * PROBES].reshape(3, PROBES) / total
    return moments, previous, current


def solution(mesh):
    sizes = mesh.shape["gx"], mesh.shape["gy"], mesh.shape["gz"]
    torus = Mesh(
        mesh.devices.reshape(sizes[0], sizes[1] // 2, 2, sizes[2] // 2, 2),
        ("gx",) + GY + GZ,
    )
    return jax.shard_map(
        per_device,
        mesh=torus,
        in_specs=(P("gx", GZ, GY), P("gx", GZ, GY)),
        out_specs=(P(), P(None, "gx", GZ, GY), P(None, "gx", GZ, GY)),
        check_vma=False,
    )
```

```python
import jax
import jax.numpy as jnp
from jax import lax
from jax.experimental import pallas as pl
from jax.experimental.pallas import tpu as pltpu
from jax.sharding import Mesh
from jax.sharding import PartitionSpec as P

PROBES = 8
LEVELS = 256
NX, NW, NY = 4, 8, 128
NZ = 4 * NW
PITCH = NZ + 8
GX = ("xa", "xb")
GY = ("ya", "yb")
GZ = ("za", "zb")
REST = GX + GZ

disorder_width = 4.0
spectral_scale = 8.4
TWO = 2.0 / spectral_scale
E_MUL = TWO * disorder_width / LEVELS
E_ADD = TWO * disorder_width * (0.5 / LEVELS - 0.5)

PLANES = 18
ROWS = 24
FRACTION = 2.0**20
SMALL = pltpu.CompilerParams(vmem_limit_bytes=24 * 1024 * 1024)


def vmem(n):
    return [pl.BlockSpec(memory_space=pltpu.VMEM)] * n


def lanes(shape):
    return lax.broadcasted_iota(jnp.int32, shape, len(shape) - 1)


def face_kernel(bits_far, levels_far, even, odd, bits, levels, done):
    copies = [
        pltpu.make_async_copy(bits_far, bits, done.at[0]),
        pltpu.make_async_copy(levels_far, levels, done.at[1]),
    ]
    for copy in copies:
        copy.start()
    for copy in copies:
        copy.wait()
    upper = lax.axis_index("xb")
    for out, first in ((even, 1 - upper), (odd, upper)):
        for i in range(3):
            out[8 * i : 8 * i + 8] = bits[first + i]
        for i in range(2):
            out[24 + 8 * i : 32 + 8 * i] = levels[2 * first + i]


def plane_list(bits, levels, below, above):
    found = []
    for x in range(-3, 7):
        if x < 0:
            found.append((below, 8 * (x + 3)))
        elif x < NX:
            found.append((bits, x))
        else:
            found.append((above, 8 * (x - 4)))
    for x in range(-2, 6):
        if x < 0:
            found.append((below, 24 + 8 * (x + 2)))
        elif x < NX:
            found.append((levels, x))
        else:
            found.append((above, 24 + 8 * (x - 4)))
    return found


def plane_tile(plane):
    ref, at = plane
    if len(ref.shape) == 3:
        return ref[at]
    return ref[at : at + NW, :]


def word_row(plane, w):
    ref, at = plane
    if len(ref.shape) == 3:
        return ref[at, w : w + 1, :]
    return ref[at + w : at + w + 1, :]


def level_kernel(bits, levels, even, odd, below, above, low, high):
    upper = lax.axis_index("xb")
    near, far = even[pl.ds(40 * (1 - upper), 40), :], odd[...]
    below[...] = jnp.where(upper == 1, near, far)
    above[...] = jnp.where(upper == 1, far, near)
    planes = plane_list(bits, levels, below, above)
    for out, w in ((low, 0), (high, NW - 1)):
        out[16:24] = jnp.zeros((8, NY), jnp.int32)
        for k, plane in enumerate(planes):
            out[k : k + 1] = word_row(plane, w)


def tiles():
    tile = (PROBES, NY)
    probe = lax.broadcasted_iota(jnp.int32, tile, 0)
    return tile, probe, lanes(tile), [jnp.left_shift(1, 4 * probe + j) for j in range(4)]


def sign_of(row, bit):
    return jnp.where((row & bit) != 0, 1.0, -1.0)


def energy_of(row, j):
    return (jnp.right_shift(row, 8 * j) & 255).astype(jnp.float32) * E_MUL + E_ADD


def step(v, energy, at, place):
    x, z = at
    own = v[x, z]
    s = pltpu.roll(own, NY - 1, 1) + pltpu.roll(own, 1, 1)
    s = s + (v[x + 1, z] + v[x - 1, z])
    s = s + (v[x, z + 1] + v[x, z - 1])
    return energy[place] * own - TWO * s


def sums_row(sums, mask, probe, lane):
    row = jnp.zeros(lane.shape, jnp.float32)
    for n, acc in enumerate(sums):
        total = jnp.sum(jnp.where(mask, acc, 0.0), axis=1, keepdims=True)
        row = jnp.where(lane == 8 * n + probe, total, row)
    return jnp.sum(row, axis=0, keepdims=True)


def add_sums(sums, v0, x, z, values):
    sign = v0[x + 3, z + 3]
    return [acc + sign * v for acc, v in zip(sums, values)]


def inner_kernel(bits, levels, below, above, strips, sums_out, v0, energy, v1, v2, v3):
    planes = plane_list(bits, levels, below, above)
    tile, probe, lane, bit_of = tiles()
    word = lax.broadcasted_iota(jnp.int32, tile, 0)
    mask = (lane // 16 == word) & (lane % 16 < 12)
    strips[16:24] = jnp.zeros((8, NY), jnp.int32)
    for k, plane in enumerate(planes):
        rolled = pltpu.roll(plane_tile(plane), 6, 1, stride=16, stride_axis=0)
        strips[k : k + 1] = jnp.sum(jnp.where(mask, rolled, 0), axis=0, keepdims=True)

    for w in range(NW):
        for k in range(10):
            row = jnp.broadcast_to(word_row(planes[k], w), tile)
            for j in range(4):
                v0[k, 4 * w + j + 3] = sign_of(row, bit_of[j])
        for k in range(8):
            row = jnp.broadcast_to(word_row(planes[10 + k], w), tile)
            for j in range(4):
                energy[k, 4 * w + j + 2] = energy_of(row, j)

    def first(i, carry):
        for u in range(2):
            x = 2 * i + u
            for z in range(3, NZ + 1):
                v1[x, z] = 0.5 * step(v0, energy, (x + 1, z + 1), (x, z))
        return carry

    lax.fori_loop(0, (NX + 4) // 2, first, 0)

    def second(i, carry):
        for u in range(2):
            x = 2 * i + u
            for z in range(3, NZ - 1):
                v2[x, z] = step(v1, energy, (x + 1, z + 1), (x + 1, z + 1)) - v0[x + 2, z + 2]
        return carry

    lax.fori_loop(0, (NX + 2) // 2, second, 0)

    def third(i, sums):
        for u in range(2):
            x = 2 * i + u
            for z in range(3, NZ - 3):
                one = v1[x + 2, z + 2]
                two = v2[x + 1, z + 1]
                three = step(v2, energy, (x + 1, z + 1), (x + 2, z + 2)) - one
                v3[x, z] = three
                sums = add_sums(sums, v0, x, z, (one, two, three))
        return tuple(sums)

    sums = lax.fori_loop(0, NX // 2, third, (jnp.zeros(tile, jnp.float32),) * 3)
    for n in range(3):
        sums_out[n] = sums[n]


def outer_kernel(
    under, over, strips_in, sums_in, v0_in, energy_in, v1_in, v2_in, v3_in,
    strips, v0, energy, v1, v2, v3,
):
    del v0_in, energy_in, v1_in, v2_in, v3_in
    tile, probe, lane, bit_of = tiles()
    strips[:ROWS] = strips_in[...]
    wide = lanes((ROWS, NY))
    strips[ROWS:] = jnp.where(
        wide < 16, pltpu.roll(under[...], 6, 1), pltpu.roll(over[...], 6 + 112, 1)
    )
    for ref, base in ((under, -4), (over, NZ)):
        for k in range(10):
            row = jnp.broadcast_to(ref[k : k + 1, :], tile)
            for j in range(4):
                if -3 <= base + j < NZ + 3:
                    v0[k, base + j + 3] = sign_of(row, bit_of[j])
        for k in range(8):
            row = jnp.broadcast_to(ref[10 + k : 11 + k, :], tile)
            for j in range(4):
                if -2 <= base + j < NZ + 2:
                    energy[k, base + j + 2] = energy_of(row, j)
    for x in range(NX + 4):
        for z in (0, 1, 2, NZ + 1, NZ + 2, NZ + 3):
            v1[x, z] = 0.5 * step(v0, energy, (x + 1, z + 1), (x, z))
    for x in range(NX + 2):
        for z in (0, 1, 2, NZ - 1, NZ, NZ + 1):
            v2[x, z] = step(v1, energy, (x + 1, z + 1), (x + 1, z + 1)) - v0[x + 2, z + 2]
    sums = [sums_in[n] for n in range(3)]
    for x in range(NX):
        for z in (0, 1, 2, NZ - 3, NZ - 2, NZ - 1):
            one = v1[x + 2, z + 2]
            two = v2[x + 1, z + 1]
            three = step(v2, energy, (x + 1, z + 1), (x + 2, z + 2)) - one
            v3[x, z] = three
            sums = add_sums(sums, v0, x, z, (one, two, three))
    row = sums_row(sums, (lane >= 3) & (lane < NY - 3), probe, lane)
    whole = row.astype(jnp.int32)
    part = (row - whole.astype(jnp.float32)) * FRACTION
    strips[PLANES : PLANES + 1] = whole
    strips[PLANES + 1 : PLANES + 2] = part.astype(jnp.int32)


def edge_kernel(
    gathered, v2, v3,
    previous, current, message,
    words, e0, energy, e1, e2, e3, blocks, done,
):
    count = gathered.shape[0] // (2 * ROWS)
    tile, probe, lane, bit_of = tiles()
    wide = lanes((ROWS, NY))

    def interfaces(i, sums):
        sums = list(sums)
        for u in range(2):
            k = 2 * i + u
            here, there = 2 * ROWS * k, 2 * ROWS * ((k + 1) % count)
            left = wide % 16 < 6
            own = jnp.where(left, gathered[pl.ds(here, ROWS), :], gathered[pl.ds(there, ROWS), :])
            far = jnp.where(
                left,
                gathered[pl.ds(here + ROWS, ROWS), :],
                gathered[pl.ds(there + ROWS, ROWS), :],
            )
            words[u, 0] = jnp.where(wide < 16, far, pltpu.roll(own, 16, 1))
            words[u, 1] = own
            words[u, 2] = jnp.where(wide >= 112, far, pltpu.roll(own, 112, 1))
        for u in range(2):
            for n in range(3):
                for k in range(10):
                    row = jnp.broadcast_to(words[u, n, k : k + 1, :], tile)
                    for j in range(4):
                        z = 4 * n - 4 + j
                        if -3 <= z < 7:
                            e0[u, k, z + 3] = sign_of(row, bit_of[j])
                for k in range(8):
                    row = jnp.broadcast_to(words[u, n, 10 + k : 11 + k, :], tile)
                    for j in range(4):
                        z = 4 * n - 4 + j
                        if -2 <= z < 6:
                            energy[u, k, z + 2] = energy_of(row, j)
        for u in range(2):
            for x in range(8):
                for z in range(8):
                    e1[u, x, z] = 0.5 * step(e0.at[u], energy.at[u], (x + 1, z + 1), (x, z))
        for u in range(2):
            for x in range(6):
                for z in range(6):
                    e2[2 * i + u, x, z] = (
                        step(e1.at[u], energy.at[u], (x + 1, z + 1), (x + 1, z + 1))
                        - e0[u, x + 2, z + 2]
                    )
        for u in range(2):
            for x in range(4):
                for z in range(4):
                    one = e1[u, x + 2, z + 2]
                    two = e2[2 * i + u, x + 1, z + 1]
                    three = (
                        step(e2.at[2 * i + u], energy.at[u], (x + 1, z + 1), (x + 2, z + 2)) - one
                    )
                    e3[2 * i + u, x, z] = three
                    sign = e0[u, x + 3, z + 3]
                    sums = [acc + sign * v for acc, v in zip(sums, (one, two, three))]
        return tuple(sums)

    sums = lax.fori_loop(0, count // 2, interfaces, (jnp.zeros(tile, jnp.float32),) * 3)

    here = 2 * lax.axis_index("ya") + lax.axis_index("yb")
    before = (here + count - 1) % count
    right = lane % 16 < 6
    outside = (lane < 3) | (lane >= NY - 3)
    rows = blocks.reshape(2 * NX * PROBES * PITCH, NY)

    def copy_out(n, x):
        return pltpu.make_async_copy(
            blocks.at[n, x, :, pl.ds(0, NZ), :], (previous, current)[n].at[:, x], done.at[n, x]
        )

    def merge(x, carry):
        for n, (main, edge, margin) in enumerate(((v2, e2, 1), (v3, e3, 0))):
            for j in range(4):
                fix = jnp.where(
                    right,
                    edge[here, x + margin, j + margin],
                    edge[before, x + margin, j + margin],
                )
                for w in range(NW):
                    z = 4 * w + j
                    moved = pltpu.roll(fix, (-16 * w - 6) % NY, 1)
                    value = jnp.where(outside, moved, main[x + margin, z + margin])
                    at = (n * NX + x) * PROBES * PITCH + z
                    rows[pl.ds(at, PROBES, stride=PITCH), :] = value
            copy_out(n, x).start()
        return carry

    lax.fori_loop(0, NX, merge, 0)

    row = sums_row(sums, (lane % 16 >= 3) & (lane % 16 < 9), probe, lane)
    for k in range(count):
        at = 2 * ROWS * k + PLANES
        whole = gathered[at : at + 1, :].astype(jnp.float32)
        part = gathered[at + 1 : at + 2, :].astype(jnp.float32)
        row = row + (whole + part * (1.0 / FRACTION))
    message[...] = jnp.broadcast_to(row, message.shape)
    for n in range(2):
        for x in range(NX):
            copy_out(n, x).wait()


def local(rows, dtype=jnp.int32):
    return pltpu.VMEM(rows, dtype)


def keep(array):
    return pltpu.with_memory_space_constraint(array, pltpu.VMEM)


def shift(array, axis, by):
    count = lax.axis_size(axis)
    return lax.ppermute(array, axis, [(i, (i + by) % count) for i in range(count)])


def per_device(bits, levels):
    f32 = jnp.float32
    face = (40, NY)
    even, odd, bits, levels = pl.pallas_call(
        face_kernel,
        out_shape=(local(face), local(face), local(bits.shape), local(levels.shape)),
        in_specs=[pl.BlockSpec(memory_space=pltpu.HBM)] * 2,
        out_specs=tuple(vmem(4)),
        scratch_shapes=[pltpu.SemaphoreType.DMA((2,))],
        name="face",
        compiler_params=SMALL,
    )(bits, levels)
    bits, levels = keep(bits), keep(levels)
    size = lax.axis_size(GX)
    across = [(i, (i + 1) % size if i % 2 else (i - 1) % size) for i in range(size)]
    odd = keep(lax.ppermute(odd, GX, across))
    even = keep(lax.all_gather(even, "xb", tiled=True))
    below, above, z_low, z_high = pl.pallas_call(
        level_kernel,
        out_shape=(local(face),) * 2 + (local((ROWS, NY)),) * 2,
        in_specs=vmem(4),
        out_specs=tuple(vmem(4)),
        name="level",
        compiler_params=SMALL,
    )(bits, levels, even, odd)
    under = keep(shift(z_high, GZ, 1))
    over = keep(shift(z_low, GZ, -1))

    def field(margin):
        return local((NX + 2 * margin, NZ + 2 * margin, PROBES, NY), f32)

    fields = [field(margin) for margin in (3, 2, 2, 1, 0)]
    strips, *inner = pl.pallas_call(
        inner_kernel,
        out_shape=(local((ROWS, NY)), local((3, PROBES, NY), f32), *fields),
        in_specs=vmem(4),
        out_specs=tuple(vmem(7)),
        name="inner",
        compiler_params=SMALL,
    )(bits, levels, keep(below), keep(above))
    inner = [keep(array) for array in (strips, *inner)]
    strips, *_, v2, v3 = pl.pallas_call(
        outer_kernel,
        out_shape=(local((2 * ROWS, NY)), *fields),
        in_specs=vmem(9),
        out_specs=tuple(vmem(6)),
        input_output_aliases={4 + i: 1 + i for i in range(5)},
        name="outer",
        compiler_params=SMALL,
    )(under, over, *inner)
    gathered = keep(lax.all_gather(strips, GY, tiled=True))
    count = lax.axis_size(GY)
    rest = lax.axis_size(REST)
    total = rest * count * NX * NZ * NY
    block = (PROBES, NX, NZ, NY)
    hbm = pl.BlockSpec(memory_space=pl.ANY)

    def edge(n, margin):
        return pltpu.VMEM((n, 4 + 2 * margin, 4 + 2 * margin, PROBES, NY), f32)

    previous, current, message = pl.pallas_call(
        edge_kernel,
        out_shape=(
            jax.ShapeDtypeStruct(block, f32),
            jax.ShapeDtypeStruct(block, f32),
            local((rest, NY), f32),
        ),
        in_specs=vmem(3),
        out_specs=(hbm, hbm, vmem(1)[0]),
        scratch_shapes=[
            pltpu.VMEM((2, 3, ROWS, NY), jnp.int32),
            edge(2, 3),
            edge(2, 2),
            edge(2, 2),
            edge(count, 1),
            edge(count, 0),
            pltpu.VMEM((2, NX, PROBES, PITCH, NY), f32),
            pltpu.SemaphoreType.DMA((2, NX)),
        ],
        name="edges",
        compiler_params=SMALL,
    )(gathered, keep(v2), keep(v3))
    summed = jnp.sum(lax.all_to_all(message, REST, 0, 0, tiled=True), axis=0)
    moments = summed[: 3 * PROBES].reshape(3, PROBES) / total
    return moments, previous, current


def solution(mesh):
    halves = [n for axis in ("gx", "gy", "gz") for n in (mesh.shape[axis] // 2, 2)]
    torus = Mesh(mesh.devices.reshape(halves), GX + GY + GZ)
    return jax.shard_map(
        per_device,
        mesh=torus,
        in_specs=(P(GX, GZ, GY), P(GX, GZ, GY)),
        out_specs=(P(), P(None, GX, GZ, GY), P(None, GX, GZ, GY)),
        check_vma=False,
    )
```

```python
import functools
import itertools

import jax
import jax.numpy as jnp
from jax import lax
from jax.experimental import pallas as pl
from jax.experimental.pallas import tpu as pltpu
from jax.sharding import Mesh
from jax.sharding import PartitionSpec as P

PROBES = 8
LEVELS = 256
NX, NW, NY = 4, 8, 128
NZ = 4 * NW
PITCH = NZ + 8
GX = ("xa", "xb")
GY = ("ya", "yb")
GZ = ("za", "zb")
REST = GX + GZ
EVERY = GX + GY + GZ

disorder_width = 4.0
spectral_scale = 8.4
TWO = 2.0 / spectral_scale
E_MUL = TWO * disorder_width / LEVELS
E_ADD = TWO * disorder_width * (0.5 / LEVELS - 0.5)

PLANES = 18
ROWS = 24
FRACTION = 2.0**20
SMALL = pltpu.CompilerParams(vmem_limit_bytes=24 * 1024 * 1024)


def vmem(n):
    return [pl.BlockSpec(memory_space=pltpu.VMEM)] * n


def lanes(shape):
    return lax.broadcasted_iota(jnp.int32, shape, len(shape) - 1)


def face_kernel(bits_far, levels_far, even, odd, bits, levels, done):
    copies = [
        pltpu.make_async_copy(bits_far, bits, done.at[0]),
        pltpu.make_async_copy(levels_far, levels, done.at[1]),
    ]
    for copy in copies:
        copy.start()
    for copy in copies:
        copy.wait()
    upper = lax.axis_index("xb")
    for out, first in ((even, 1 - upper), (odd, upper)):
        for i in range(3):
            out[8 * i : 8 * i + 8] = bits[first + i]
        for i in range(2):
            out[24 + 8 * i : 32 + 8 * i] = levels[2 * first + i]


def plane_list(bits, levels, below, above):
    found = []
    for x in range(-3, 7):
        if x < 0:
            found.append((below, 8 * (x + 3)))
        elif x < NX:
            found.append((bits, x))
        else:
            found.append((above, 8 * (x - 4)))
    for x in range(-2, 6):
        if x < 0:
            found.append((below, 24 + 8 * (x + 2)))
        elif x < NX:
            found.append((levels, x))
        else:
            found.append((above, 24 + 8 * (x - 4)))
    return found


def plane_tile(plane):
    ref, at = plane
    if len(ref.shape) == 3:
        return ref[at]
    return ref[at : at + NW, :]


def word_row(plane, w):
    ref, at = plane
    if len(ref.shape) == 3:
        return ref[at, w : w + 1, :]
    return ref[at + w : at + w + 1, :]


def level_kernel(bits, levels, even, odd, below, above, low, high):
    upper = lax.axis_index("xb")
    near, far = even[pl.ds(40 * (1 - upper), 40), :], odd[...]
    below[...] = jnp.where(upper == 1, near, far)
    above[...] = jnp.where(upper == 1, far, near)
    planes = plane_list(bits, levels, below, above)
    for out, w in ((low, 0), (high, NW - 1)):
        out[16:24] = jnp.zeros((8, NY), jnp.int32)
        for k, plane in enumerate(planes):
            out[k : k + 1] = word_row(plane, w)


def tiles():
    tile = (PROBES, NY)
    probe = lax.broadcasted_iota(jnp.int32, tile, 0)
    return tile, probe, lanes(tile), [jnp.left_shift(1, 4 * probe + j) for j in range(4)]


def sign_of(row, bit):
    return jnp.where((row & bit) != 0, 1.0, -1.0)


def energy_of(row, j):
    return (jnp.right_shift(row, 8 * j) & 255).astype(jnp.float32) * E_MUL + E_ADD


def step(v, energy, at, place):
    x, z = at
    own = v[x, z]
    s = pltpu.roll(own, NY - 1, 1) + pltpu.roll(own, 1, 1)
    s = s + (v[x + 1, z] + v[x - 1, z])
    s = s + (v[x, z + 1] + v[x, z - 1])
    return energy[place] * own - TWO * s


def sums_row(sums, mask, probe, lane):
    row = jnp.zeros(lane.shape, jnp.float32)
    for n, acc in enumerate(sums):
        total = jnp.sum(jnp.where(mask, acc, 0.0), axis=1, keepdims=True)
        row = jnp.where(lane == 8 * n + probe, total, row)
    return jnp.sum(row, axis=0, keepdims=True)


def add_sums(sums, v0, x, z, values):
    sign = v0[x + 3, z + 3]
    return [acc + sign * v for acc, v in zip(sums, values)]


def inner_kernel(bits, levels, below, above, strips, sums_out, v0, energy, v1, v2, v3):
    planes = plane_list(bits, levels, below, above)
    tile, probe, lane, bit_of = tiles()
    word = lax.broadcasted_iota(jnp.int32, tile, 0)
    mask = (lane // 16 == word) & (lane % 16 < 12)
    strips[16:24] = jnp.zeros((8, NY), jnp.int32)
    for k, plane in enumerate(planes):
        rolled = pltpu.roll(plane_tile(plane), 6, 1, stride=16, stride_axis=0)
        strips[k : k + 1] = jnp.sum(jnp.where(mask, rolled, 0), axis=0, keepdims=True)

    for w in range(NW):
        for k in range(10):
            row = jnp.broadcast_to(word_row(planes[k], w), tile)
            for j in range(4):
                v0[k, 4 * w + j + 3] = sign_of(row, bit_of[j])
        for k in range(8):
            row = jnp.broadcast_to(word_row(planes[10 + k], w), tile)
            for j in range(4):
                energy[k, 4 * w + j + 2] = energy_of(row, j)

    def first(i, carry):
        for u in range(2):
            x = 2 * i + u
            for z in range(3, NZ + 1):
                v1[x, z] = 0.5 * step(v0, energy, (x + 1, z + 1), (x, z))
        return carry

    lax.fori_loop(0, (NX + 4) // 2, first, 0)

    def second(i, carry):
        for u in range(2):
            x = 2 * i + u
            for z in range(3, NZ - 1):
                v2[x, z] = step(v1, energy, (x + 1, z + 1), (x + 1, z + 1)) - v0[x + 2, z + 2]
        return carry

    lax.fori_loop(0, (NX + 2) // 2, second, 0)

    def third(i, sums):
        for u in range(2):
            x = 2 * i + u
            for z in range(3, NZ - 3):
                one = v1[x + 2, z + 2]
                two = v2[x + 1, z + 1]
                three = step(v2, energy, (x + 1, z + 1), (x + 2, z + 2)) - one
                v3[x, z] = three
                sums = add_sums(sums, v0, x, z, (one, two, three))
        return tuple(sums)

    sums = lax.fori_loop(0, NX // 2, third, (jnp.zeros(tile, jnp.float32),) * 3)
    for n in range(3):
        sums_out[n] = sums[n]


def outer_kernel(
    under, over, strips_in, sums_in, v0_in, energy_in, v1_in, v2_in, v3_in,
    strips, v0, energy, v1, v2, v3,
):
    del v0_in, energy_in, v1_in, v2_in, v3_in
    tile, probe, lane, bit_of = tiles()
    strips[:ROWS] = strips_in[...]
    wide = lanes((ROWS, NY))
    strips[ROWS:] = jnp.where(
        wide < 16, pltpu.roll(under[...], 6, 1), pltpu.roll(over[...], 6 + 112, 1)
    )
    for ref, base in ((under, -4), (over, NZ)):
        for k in range(10):
            row = jnp.broadcast_to(ref[k : k + 1, :], tile)
            for j in range(4):
                if -3 <= base + j < NZ + 3:
                    v0[k, base + j + 3] = sign_of(row, bit_of[j])
        for k in range(8):
            row = jnp.broadcast_to(ref[10 + k : 11 + k, :], tile)
            for j in range(4):
                if -2 <= base + j < NZ + 2:
                    energy[k, base + j + 2] = energy_of(row, j)
    for x in range(NX + 4):
        for z in (0, 1, 2, NZ + 1, NZ + 2, NZ + 3):
            v1[x, z] = 0.5 * step(v0, energy, (x + 1, z + 1), (x, z))
    for x in range(NX + 2):
        for z in (0, 1, 2, NZ - 1, NZ, NZ + 1):
            v2[x, z] = step(v1, energy, (x + 1, z + 1), (x + 1, z + 1)) - v0[x + 2, z + 2]
    sums = [sums_in[n] for n in range(3)]
    for x in range(NX):
        for z in (0, 1, 2, NZ - 3, NZ - 2, NZ - 1):
            one = v1[x + 2, z + 2]
            two = v2[x + 1, z + 1]
            three = step(v2, energy, (x + 1, z + 1), (x + 2, z + 2)) - one
            v3[x, z] = three
            sums = add_sums(sums, v0, x, z, (one, two, three))
    row = sums_row(sums, (lane >= 3) & (lane < NY - 3), probe, lane)
    whole = row.astype(jnp.int32)
    part = (row - whole.astype(jnp.float32)) * FRACTION
    strips[PLANES : PLANES + 1] = whole
    strips[PLANES + 1 : PLANES + 2] = part.astype(jnp.int32)


def edge_kernel(
    gathered, v2, v3,
    previous, current, message,
    words, e0, energy, e1, e2, e3, partial, blocks, done,
):
    count = gathered.shape[0] // (2 * ROWS)
    tile, probe, lane, bit_of = tiles()
    wide = lanes((ROWS, NY))

    place = 2 * lax.axis_index("ya") + lax.axis_index("yb")
    first = place + count - 1

    def interfaces(i, carry):
        for u in range(2):
            k = (first + 2 * i + u) % count
            here, there = 2 * ROWS * k, 2 * ROWS * ((k + 1) % count)
            left = wide % 16 < 6
            own = jnp.where(left, gathered[pl.ds(here, ROWS), :], gathered[pl.ds(there, ROWS), :])
            far = jnp.where(
                left,
                gathered[pl.ds(here + ROWS, ROWS), :],
                gathered[pl.ds(there + ROWS, ROWS), :],
            )
            words[u, 0] = jnp.where(wide < 16, far, pltpu.roll(own, 16, 1))
            words[u, 1] = own
            words[u, 2] = jnp.where(wide >= 112, far, pltpu.roll(own, 112, 1))
        for u in range(2):
            for n in range(3):
                for k in range(10):
                    row = jnp.broadcast_to(words[u, n, k : k + 1, :], tile)
                    for j in range(4):
                        z = 4 * n - 4 + j
                        if -3 <= z < 7:
                            e0[u, k, z + 3] = sign_of(row, bit_of[j])
                for k in range(8):
                    row = jnp.broadcast_to(words[u, n, 10 + k : 11 + k, :], tile)
                    for j in range(4):
                        z = 4 * n - 4 + j
                        if -2 <= z < 6:
                            energy[u, k, z + 2] = energy_of(row, j)
        for u in range(2):
            for x in range(8):
                for z in range(8):
                    e1[u, x, z] = 0.5 * step(e0.at[u], energy.at[u], (x + 1, z + 1), (x, z))
        for u in range(2):
            for x in range(6):
                for z in range(6):
                    e2[2 * i + u, x, z] = (
                        step(e1.at[u], energy.at[u], (x + 1, z + 1), (x + 1, z + 1))
                        - e0[u, x + 2, z + 2]
                    )
        for u in range(2):
            sums = (jnp.zeros(tile, jnp.float32),) * 3
            for x in range(4):
                for z in range(4):
                    one = e1[u, x + 2, z + 2]
                    two = e2[2 * i + u, x + 1, z + 1]
                    three = (
                        step(e2.at[2 * i + u], energy.at[u], (x + 1, z + 1), (x + 2, z + 2)) - one
                    )
                    e3[2 * i + u, x, z] = three
                    sums = add_sums(sums, e0.at[u], x, z, (one, two, three))
            for n in range(3):
                partial[(first + 2 * i + u) % count, n] = sums[n]

        @pl.when(i == 0)
        def _():
            lax.fori_loop(0, NX, merge, 0)

        return carry

    right = lane % 16 < 6
    outside = (lane < 3) | (lane >= NY - 3)
    rows = blocks.reshape(2 * NX * PROBES * PITCH, NY)

    def copy_out(n, x):
        return pltpu.make_async_copy(
            blocks.at[n, x, :, pl.ds(0, NZ), :], (previous, current)[n].at[:, x], done.at[n, x]
        )

    def merge(x, carry):
        for n, (main, edge, margin) in enumerate(((v2, e2, 1), (v3, e3, 0))):
            for j in range(4):
                fix = jnp.where(
                    right,
                    edge[1, x + margin, j + margin],
                    edge[0, x + margin, j + margin],
                )
                for w in range(NW):
                    z = 4 * w + j
                    moved = pltpu.roll(fix, (-16 * w - 6) % NY, 1)
                    value = jnp.where(outside, moved, main[x + margin, z + margin])
                    at = (n * NX + x) * PROBES * PITCH + z
                    rows[pl.ds(at, PROBES, stride=PITCH), :] = value
            copy_out(n, x).start()
        return carry

    lax.fori_loop(0, count // 2, interfaces, 0)
    sums = [sum((partial[k, n] for k in range(1, count)), partial[0, n]) for n in range(3)]
    row = sums_row(sums, (lane % 16 >= 3) & (lane % 16 < 9), probe, lane)
    for k in range(count):
        at = 2 * ROWS * k + PLANES
        whole = gathered[at : at + 1, :].astype(jnp.float32)
        part = gathered[at + 1 : at + 2, :].astype(jnp.float32)
        row = row + (whole + part * (1.0 / FRACTION))
    message[...] = jnp.broadcast_to(row, message.shape)
    for n in range(2):
        for x in range(NX):
            copy_out(n, x).wait()


def moment_kernel(parts, moments, *, scale):
    row = jnp.sum(parts[...], axis=0, keepdims=True) * scale
    for n in range(3):
        moments[n : n + 1, :] = pltpu.roll(row, (-8 * n) % NY, 1)[:, :PROBES]


def local(rows, dtype=jnp.int32):
    return pltpu.VMEM(rows, dtype)


def keep(array):
    return pltpu.with_memory_space_constraint(array, pltpu.VMEM)


def far(array):
    return pltpu.with_memory_space_constraint(array, pltpu.HBM)


def shift(array, axis, by):
    count = lax.axis_size(axis)
    return lax.ppermute(array, axis, [(i, (i + by) % count) for i in range(count)])


def groups():
    sizes = [lax.axis_size(axis) for axis in EVERY]
    found = {}
    for index, (xa, xb, ya, yb, za, zb) in enumerate(itertools.product(*map(range, sizes))):
        found.setdefault(((ya + zb) % sizes[2], yb), []).append(((xa, xb, za, zb), index))
    return [[index for _, index in sorted(members)] for members in found.values()]


def per_device(bits, levels):
    f32 = jnp.float32
    face = (40, NY)
    even, odd, bits, levels = pl.pallas_call(
        face_kernel,
        out_shape=(local(face), local(face), local(bits.shape), local(levels.shape)),
        in_specs=[pl.BlockSpec(memory_space=pltpu.HBM)] * 2,
        out_specs=tuple(vmem(4)),
        scratch_shapes=[pltpu.SemaphoreType.DMA((2,))],
        name="face",
        compiler_params=SMALL,
    )(far(bits), far(levels))
    bits, levels = keep(bits), keep(levels)
    size = lax.axis_size(GX)
    across = [(i, (i + 1) % size if i % 2 else (i - 1) % size) for i in range(size)]
    odd = keep(lax.ppermute(odd, GX, across))
    even = keep(lax.all_gather(even, "xb", tiled=True))
    below, above, z_low, z_high = pl.pallas_call(
        level_kernel,
        out_shape=(local(face),) * 2 + (local((ROWS, NY)),) * 2,
        in_specs=vmem(4),
        out_specs=tuple(vmem(4)),
        name="level",
        compiler_params=SMALL,
    )(bits, levels, even, odd)
    under = keep(shift(z_high, GZ, 1))
    over = keep(shift(z_low, GZ, -1))

    def field(margin):
        return local((NX + 2 * margin, NZ + 2 * margin, PROBES, NY), f32)

    fields = [field(margin) for margin in (3, 2, 2, 1, 0)]
    strips, *inner = pl.pallas_call(
        inner_kernel,
        out_shape=(local((ROWS, NY)), local((3, PROBES, NY), f32), *fields),
        in_specs=vmem(4),
        out_specs=tuple(vmem(7)),
        name="inner",
        compiler_params=SMALL,
    )(bits, levels, keep(below), keep(above))
    inner = [keep(array) for array in (strips, *inner)]
    strips, *_, v2, v3 = pl.pallas_call(
        outer_kernel,
        out_shape=(local((2 * ROWS, NY)), *fields),
        in_specs=vmem(9),
        out_specs=tuple(vmem(6)),
        input_output_aliases={4 + i: 1 + i for i in range(5)},
        name="outer",
        compiler_params=SMALL,
    )(under, over, *inner)
    gathered = keep(lax.all_gather(strips, GY, tiled=True))
    count = lax.axis_size(GY)
    rest = lax.axis_size(REST)
    total = rest * count * NX * NZ * NY
    block = (PROBES, NX, NZ, NY)
    hbm = pl.BlockSpec(memory_space=pl.ANY)

    def edge(n, margin):
        return pltpu.VMEM((n, 4 + 2 * margin, 4 + 2 * margin, PROBES, NY), f32)

    previous, current, message = pl.pallas_call(
        edge_kernel,
        out_shape=(
            jax.ShapeDtypeStruct(block, f32),
            jax.ShapeDtypeStruct(block, f32),
            local((rest, NY), f32),
        ),
        in_specs=vmem(3),
        out_specs=(hbm, hbm, vmem(1)[0]),
        scratch_shapes=[
            pltpu.VMEM((2, 3, ROWS, NY), jnp.int32),
            edge(2, 3),
            edge(2, 2),
            edge(2, 2),
            edge(count, 1),
            edge(count, 0),
            pltpu.VMEM((count, 3, PROBES, NY), f32),
            pltpu.VMEM((2, NX, PROBES, PITCH, NY), f32),
            pltpu.SemaphoreType.DMA((2, NX)),
        ],
        name="edges",
        compiler_params=SMALL,
    )(gathered, keep(v2), keep(v3))
    parts = lax.all_to_all(message, EVERY, 0, 0, axis_index_groups=groups(), tiled=True)
    moments = pl.pallas_call(
        functools.partial(moment_kernel, scale=1.0 / total),
        out_shape=jax.ShapeDtypeStruct((3, PROBES), f32),
        in_specs=vmem(1),
        out_specs=vmem(1)[0],
        name="moment",
        compiler_params=SMALL,
    )(keep(parts))
    return moments, previous, current


def solution(mesh):
    halves = [n for axis in ("gx", "gy", "gz") for n in (mesh.shape[axis] // 2, 2)]
    torus = Mesh(mesh.devices.reshape(halves), GX + GY + GZ)
    return jax.shard_map(
        per_device,
        mesh=torus,
        in_specs=(P(GX, GZ, GY), P(GX, GZ, GY)),
        out_specs=(P(), P(None, GX, GZ, GY), P(None, GX, GZ, GY)),
        check_vma=False,
    )
```

```python
import functools
import itertools

import jax
import jax.numpy as jnp
from jax import lax
from jax.experimental import pallas as pl
from jax.experimental.pallas import tpu as pltpu
from jax.sharding import Mesh
from jax.sharding import PartitionSpec as P

PROBES = 8
LEVELS = 256
NX, NW, NY = 4, 8, 128
NZ = 4 * NW
PITCH = NZ + 8
GX = ("xa", "xb")
GY = ("ya", "yb")
GZ = ("za", "zb")
REST = GX + GZ
EVERY = GX + GY + GZ

disorder_width = 4.0
spectral_scale = 8.4
TWO = 2.0 / spectral_scale
E_MUL = TWO * disorder_width / LEVELS
E_ADD = TWO * disorder_width * (0.5 / LEVELS - 0.5)

PLANES = 18
ROWS = 24
FRACTION = 2.0**20
SMALL = pltpu.CompilerParams(vmem_limit_bytes=24 * 1024 * 1024)


def vmem(n):
    return [pl.BlockSpec(memory_space=pltpu.VMEM)] * n


def lanes(shape):
    return lax.broadcasted_iota(jnp.int32, shape, len(shape) - 1)


def face_kernel(bits_far, levels_far, even, odd, bits, levels, done):
    copies = [
        pltpu.make_async_copy(bits_far, bits, done.at[0]),
        pltpu.make_async_copy(levels_far, levels, done.at[1]),
    ]
    for copy in copies:
        copy.start()
    for copy in copies:
        copy.wait()
    upper = lax.axis_index("xb")
    for out, first in ((even, 1 - upper), (odd, upper)):
        for i in range(3):
            out[8 * i : 8 * i + 8] = bits[first + i]
        for i in range(2):
            out[24 + 8 * i : 32 + 8 * i] = levels[2 * first + i]


def plane_list(bits, levels, below, above):
    found = []
    for x in range(-3, 7):
        if x < 0:
            found.append((below, 8 * (x + 3)))
        elif x < NX:
            found.append((bits, x))
        else:
            found.append((above, 8 * (x - 4)))
    for x in range(-2, 6):
        if x < 0:
            found.append((below, 24 + 8 * (x + 2)))
        elif x < NX:
            found.append((levels, x))
        else:
            found.append((above, 24 + 8 * (x - 4)))
    return found


def plane_tile(plane):
    ref, at = plane
    if len(ref.shape) == 3:
        return ref[at]
    return ref[at : at + NW, :]


def word_row(plane, w):
    ref, at = plane
    if len(ref.shape) == 3:
        return ref[at, w : w + 1, :]
    return ref[at + w : at + w + 1, :]


def level_kernel(bits, levels, even, odd, below, above, z_even, z_odd, low, high):
    upper = lax.axis_index("xb")
    near, far = even[pl.ds(40 * (1 - upper), 40), :], odd[...]
    below[...] = jnp.where(upper == 1, near, far)
    above[...] = jnp.where(upper == 1, far, near)
    planes = plane_list(bits, levels, below, above)
    for out, w in ((low, 0), (high, NW - 1)):
        out[16:24] = jnp.zeros((8, NY), jnp.int32)
        for k, plane in enumerate(planes):
            out[k : k + 1] = word_row(plane, w)
    up = lax.axis_index("zb") == 0
    z_even[...] = jnp.where(up, high[...], low[...])
    z_odd[...] = jnp.where(up, low[...], high[...])


def tiles():
    tile = (PROBES, NY)
    probe = lax.broadcasted_iota(jnp.int32, tile, 0)
    return tile, probe, lanes(tile), [jnp.left_shift(1, 4 * probe + j) for j in range(4)]


def sign_of(row, bit):
    return jnp.where((row & bit) != 0, 1.0, -1.0)


def energy_of(row, j):
    return (jnp.right_shift(row, 8 * j) & 255).astype(jnp.float32) * E_MUL + E_ADD


def step(v, energy, at, place):
    x, z = at
    own = v[x, z]
    s = pltpu.roll(own, NY - 1, 1) + pltpu.roll(own, 1, 1)
    s = s + (v[x + 1, z] + v[x - 1, z])
    s = s + (v[x, z + 1] + v[x, z - 1])
    return energy[place] * own - TWO * s


def sums_row(sums, mask, probe, lane):
    row = jnp.zeros(lane.shape, jnp.float32)
    for n, acc in enumerate(sums):
        total = jnp.sum(jnp.where(mask, acc, 0.0), axis=1, keepdims=True)
        row = jnp.where(lane == 8 * n + probe, total, row)
    return jnp.sum(row, axis=0, keepdims=True)


def add_sums(sums, v0, x, z, values):
    sign = v0[x + 3, z + 3]
    return [acc + sign * v for acc, v in zip(sums, values)]


def inner_kernel(bits, levels, below, above, strips, sums_out, v0, energy, v1, v2, v3):
    planes = plane_list(bits, levels, below, above)
    tile, probe, lane, bit_of = tiles()
    word = lax.broadcasted_iota(jnp.int32, tile, 0)
    mask = (lane // 16 == word) & (lane % 16 < 12)
    strips[16:24] = jnp.zeros((8, NY), jnp.int32)
    for k, plane in enumerate(planes):
        rolled = pltpu.roll(plane_tile(plane), 6, 1, stride=16, stride_axis=0)
        strips[k : k + 1] = jnp.sum(jnp.where(mask, rolled, 0), axis=0, keepdims=True)

    for w in range(NW):
        for k in range(10):
            row = jnp.broadcast_to(word_row(planes[k], w), tile)
            for j in range(4):
                v0[k, 4 * w + j + 3] = sign_of(row, bit_of[j])
        for k in range(8):
            row = jnp.broadcast_to(word_row(planes[10 + k], w), tile)
            for j in range(4):
                energy[k, 4 * w + j + 2] = energy_of(row, j)

    def first(i, carry):
        for u in range(2):
            x = 2 * i + u
            for z in range(3, NZ + 1):
                v1[x, z] = 0.5 * step(v0, energy, (x + 1, z + 1), (x, z))
        return carry

    lax.fori_loop(0, (NX + 4) // 2, first, 0)

    def second(i, carry):
        for u in range(2):
            x = 2 * i + u
            for z in range(3, NZ - 1):
                v2[x, z] = step(v1, energy, (x + 1, z + 1), (x + 1, z + 1)) - v0[x + 2, z + 2]
        return carry

    lax.fori_loop(0, (NX + 2) // 2, second, 0)

    def third(i, sums):
        for u in range(2):
            x = 2 * i + u
            for z in range(3, NZ - 3):
                one = v1[x + 2, z + 2]
                two = v2[x + 1, z + 1]
                three = step(v2, energy, (x + 1, z + 1), (x + 2, z + 2)) - one
                v3[x, z] = three
                sums = add_sums(sums, v0, x, z, (one, two, three))
        return tuple(sums)

    sums = lax.fori_loop(0, NX // 2, third, (jnp.zeros(tile, jnp.float32),) * 3)
    for n in range(3):
        sums_out[n] = sums[n]


def outer_kernel(
    z_even, z_odd, strips_in, sums_in, v0_in, energy_in, v1_in, v2_in, v3_in,
    strips, v0, energy, v1, v2, v3,
    under, over,
):
    up = lax.axis_index("zb") == 0
    under[...] = jnp.where(up, z_odd[...], z_even[...])
    over[...] = jnp.where(up, z_even[...], z_odd[...])
    del v0_in, energy_in, v1_in, v2_in, v3_in
    tile, probe, lane, bit_of = tiles()
    strips[:ROWS] = strips_in[...]
    wide = lanes((ROWS, NY))
    strips[ROWS:] = jnp.where(
        wide < 16, pltpu.roll(under[...], 6, 1), pltpu.roll(over[...], 6 + 112, 1)
    )
    for ref, base in ((under, -4), (over, NZ)):
        for k in range(10):
            row = jnp.broadcast_to(ref[k : k + 1, :], tile)
            for j in range(4):
                if -3 <= base + j < NZ + 3:
                    v0[k, base + j + 3] = sign_of(row, bit_of[j])
        for k in range(8):
            row = jnp.broadcast_to(ref[10 + k : 11 + k, :], tile)
            for j in range(4):
                if -2 <= base + j < NZ + 2:
                    energy[k, base + j + 2] = energy_of(row, j)
    for x in range(NX + 4):
        for z in (0, 1, 2, NZ + 1, NZ + 2, NZ + 3):
            v1[x, z] = 0.5 * step(v0, energy, (x + 1, z + 1), (x, z))
    for x in range(NX + 2):
        for z in (0, 1, 2, NZ - 1, NZ, NZ + 1):
            v2[x, z] = step(v1, energy, (x + 1, z + 1), (x + 1, z + 1)) - v0[x + 2, z + 2]
    sums = [sums_in[n] for n in range(3)]
    for x in range(NX):
        for z in (0, 1, 2, NZ - 3, NZ - 2, NZ - 1):
            one = v1[x + 2, z + 2]
            two = v2[x + 1, z + 1]
            three = step(v2, energy, (x + 1, z + 1), (x + 2, z + 2)) - one
            v3[x, z] = three
            sums = add_sums(sums, v0, x, z, (one, two, three))
    row = sums_row(sums, (lane >= 3) & (lane < NY - 3), probe, lane)
    whole = row.astype(jnp.int32)
    part = (row - whole.astype(jnp.float32)) * FRACTION
    strips[PLANES : PLANES + 1] = whole
    strips[PLANES + 1 : PLANES + 2] = part.astype(jnp.int32)


def edge_kernel(
    gathered, v2, v3,
    previous, current, message,
    words, e0, energy, e1, e2, e3, partial, blocks, done,
):
    count = gathered.shape[0] // (2 * ROWS)
    tile, probe, lane, bit_of = tiles()
    wide = lanes((ROWS, NY))

    place = 2 * lax.axis_index("ya") + lax.axis_index("yb")
    first = place + count - 1

    def interfaces(i, carry):
        for u in range(2):
            k = (first + 2 * i + u) % count
            here, there = 2 * ROWS * k, 2 * ROWS * ((k + 1) % count)
            left = wide % 16 < 6
            own = jnp.where(left, gathered[pl.ds(here, ROWS), :], gathered[pl.ds(there, ROWS), :])
            far = jnp.where(
                left,
                gathered[pl.ds(here + ROWS, ROWS), :],
                gathered[pl.ds(there + ROWS, ROWS), :],
            )
            words[u, 0] = jnp.where(wide < 16, far, pltpu.roll(own, 16, 1))
            words[u, 1] = own
            words[u, 2] = jnp.where(wide >= 112, far, pltpu.roll(own, 112, 1))
        for u in range(2):
            for n in range(3):
                for k in range(10):
                    row = jnp.broadcast_to(words[u, n, k : k + 1, :], tile)
                    for j in range(4):
                        z = 4 * n - 4 + j
                        if -3 <= z < 7:
                            e0[u, k, z + 3] = sign_of(row, bit_of[j])
                for k in range(8):
                    row = jnp.broadcast_to(words[u, n, 10 + k : 11 + k, :], tile)
                    for j in range(4):
                        z = 4 * n - 4 + j
                        if -2 <= z < 6:
                            energy[u, k, z + 2] = energy_of(row, j)
        for u in range(2):
            for x in range(8):
                for z in range(8):
                    e1[u, x, z] = 0.5 * step(e0.at[u], energy.at[u], (x + 1, z + 1), (x, z))
        for u in range(2):
            for x in range(6):
                for z in range(6):
                    e2[2 * i + u, x, z] = (
                        step(e1.at[u], energy.at[u], (x + 1, z + 1), (x + 1, z + 1))
                        - e0[u, x + 2, z + 2]
                    )
        for u in range(2):
            sums = (jnp.zeros(tile, jnp.float32),) * 3
            for x in range(4):
                for z in range(4):
                    one = e1[u, x + 2, z + 2]
                    two = e2[2 * i + u, x + 1, z + 1]
                    three = (
                        step(e2.at[2 * i + u], energy.at[u], (x + 1, z + 1), (x + 2, z + 2)) - one
                    )
                    e3[2 * i + u, x, z] = three
                    sums = add_sums(sums, e0.at[u], x, z, (one, two, three))
            for n in range(3):
                partial[(first + 2 * i + u) % count, n] = sums[n]

        @pl.when(i == 0)
        def _():
            lax.fori_loop(0, NX, merge, 0)

        return carry

    right = lane % 16 < 6
    outside = (lane < 3) | (lane >= NY - 3)
    rows = blocks.reshape(2 * NX * PROBES * PITCH, NY)

    def copy_out(n, x):
        return pltpu.make_async_copy(
            blocks.at[n, x, :, pl.ds(0, NZ), :], (previous, current)[n].at[:, x], done.at[n, x]
        )

    def merge(x, carry):
        for n, (main, edge, margin) in enumerate(((v2, e2, 1), (v3, e3, 0))):
            for j in range(4):
                fix = jnp.where(
                    right,
                    edge[1, x + margin, j + margin],
                    edge[0, x + margin, j + margin],
                )
                for w in range(NW):
                    z = 4 * w + j
                    moved = pltpu.roll(fix, (-16 * w - 6) % NY, 1)
                    value = jnp.where(outside, moved, main[x + margin, z + margin])
                    at = (n * NX + x) * PROBES * PITCH + z
                    rows[pl.ds(at, PROBES, stride=PITCH), :] = value
            copy_out(n, x).start()
        return carry

    lax.fori_loop(0, count // 2, interfaces, 0)
    sums = [sum((partial[k, n] for k in range(1, count)), partial[0, n]) for n in range(3)]
    row = sums_row(sums, (lane % 16 >= 3) & (lane % 16 < 9), probe, lane)
    for k in range(count):
        at = 2 * ROWS * k + PLANES
        whole = gathered[at : at + 1, :].astype(jnp.float32)
        part = gathered[at + 1 : at + 2, :].astype(jnp.float32)
        row = row + (whole + part * (1.0 / FRACTION))
    message[...] = jnp.broadcast_to(row, message.shape)
    for n in range(2):
        for x in range(NX):
            copy_out(n, x).wait()


def moment_kernel(parts, moments, *, scale):
    row = jnp.sum(parts[...], axis=0, keepdims=True) * scale
    for n in range(3):
        moments[n : n + 1, :] = pltpu.roll(row, (-8 * n) % NY, 1)[:, :PROBES]


def local(rows, dtype=jnp.int32):
    return pltpu.VMEM(rows, dtype)


def keep(array):
    return pltpu.with_memory_space_constraint(array, pltpu.VMEM)


def far(array):
    return pltpu.with_memory_space_constraint(array, pltpu.HBM)


def across(axis):
    size = lax.axis_size(axis)
    return [(i, (i + 1) % size if i % 2 else (i - 1) % size) for i in range(size)]


def groups():
    sizes = [lax.axis_size(axis) for axis in EVERY]
    found = {}
    for index, (xa, xb, ya, yb, za, zb) in enumerate(itertools.product(*map(range, sizes))):
        found.setdefault(((ya + zb) % sizes[2], yb), []).append(
            (((2 * xa + xb + za) % sizes[4], xa, xb, zb), index)
        )
    return [[index for _, index in sorted(members)] for members in found.values()]


def per_device(bits, levels):
    f32 = jnp.float32
    face = (40, NY)
    even, odd, bits, levels = pl.pallas_call(
        face_kernel,
        out_shape=(local(face), local(face), local(bits.shape), local(levels.shape)),
        in_specs=[pl.BlockSpec(memory_space=pltpu.HBM)] * 2,
        out_specs=tuple(vmem(4)),
        scratch_shapes=[pltpu.SemaphoreType.DMA((2,))],
        name="face",
        compiler_params=SMALL,
    )(far(bits), far(levels))
    bits, levels = keep(bits), keep(levels)
    odd = keep(lax.ppermute(odd, GX, across(GX)))
    even = keep(lax.all_gather(even, "xb", tiled=True))
    below, above, z_even, z_odd = pl.pallas_call(
        level_kernel,
        out_shape=(local(face),) * 2 + (local((ROWS, NY)),) * 2,
        in_specs=vmem(4),
        out_specs=tuple(vmem(4)),
        scratch_shapes=[pltpu.VMEM((ROWS, NY), jnp.int32)] * 2,
        name="level",
        compiler_params=SMALL,
    )(bits, levels, even, odd)
    z_odd = keep(lax.ppermute(z_odd, GZ, across(GZ)))
    z_even = keep(lax.ppermute(z_even, "zb", [(0, 1), (1, 0)]))

    def field(margin):
        return local((NX + 2 * margin, NZ + 2 * margin, PROBES, NY), f32)

    fields = [field(margin) for margin in (3, 2, 2, 1, 0)]
    strips, *inner = pl.pallas_call(
        inner_kernel,
        out_shape=(local((ROWS, NY)), local((3, PROBES, NY), f32), *fields),
        in_specs=vmem(4),
        out_specs=tuple(vmem(7)),
        name="inner",
        compiler_params=SMALL,
    )(bits, levels, keep(below), keep(above))
    inner = [keep(array) for array in (strips, *inner)]
    strips, *_, v2, v3 = pl.pallas_call(
        outer_kernel,
        out_shape=(local((2 * ROWS, NY)), *fields),
        in_specs=vmem(9),
        out_specs=tuple(vmem(6)),
        input_output_aliases={4 + i: 1 + i for i in range(5)},
        scratch_shapes=[pltpu.VMEM((ROWS, NY), jnp.int32)] * 2,
        name="outer",
        compiler_params=SMALL,
    )(z_even, z_odd, *inner)
    gathered = keep(lax.all_gather(strips, GY, tiled=True))
    count = lax.axis_size(GY)
    rest = lax.axis_size(REST)
    total = rest * count * NX * NZ * NY
    block = (PROBES, NX, NZ, NY)
    hbm = pl.BlockSpec(memory_space=pl.ANY)

    def edge(n, margin):
        return pltpu.VMEM((n, 4 + 2 * margin, 4 + 2 * margin, PROBES, NY), f32)

    previous, current, message = pl.pallas_call(
        edge_kernel,
        out_shape=(
            jax.ShapeDtypeStruct(block, f32),
            jax.ShapeDtypeStruct(block, f32),
            local((rest, NY), f32),
        ),
        in_specs=vmem(3),
        out_specs=(hbm, hbm, vmem(1)[0]),
        scratch_shapes=[
            pltpu.VMEM((2, 3, ROWS, NY), jnp.int32),
            edge(2, 3),
            edge(2, 2),
            edge(2, 2),
            edge(count, 1),
            edge(count, 0),
            pltpu.VMEM((count, 3, PROBES, NY), f32),
            pltpu.VMEM((2, NX, PROBES, PITCH, NY), f32),
            pltpu.SemaphoreType.DMA((2, NX)),
        ],
        name="edges",
        compiler_params=SMALL,
    )(gathered, keep(v2), keep(v3))
    parts = lax.all_to_all(message, EVERY, 0, 0, axis_index_groups=groups(), tiled=True)
    moments = pl.pallas_call(
        functools.partial(moment_kernel, scale=1.0 / total),
        out_shape=jax.ShapeDtypeStruct((3, PROBES), f32),
        in_specs=vmem(1),
        out_specs=vmem(1)[0],
        name="moment",
        compiler_params=SMALL,
    )(keep(parts))
    return moments, previous, current


def solution(mesh):
    halves = [n for axis in ("gx", "gy", "gz") for n in (mesh.shape[axis] // 2, 2)]
    torus = Mesh(mesh.devices.reshape(halves), GX + GY + GZ)
    return jax.shard_map(
        per_device,
        mesh=torus,
        in_specs=(P(GX, GZ, GY), P(GX, GZ, GY)),
        out_specs=(P(), P(None, GX, GZ, GY), P(None, GX, GZ, GY)),
        check_vma=False,
    )
```

```python
import functools
import itertools

import jax
import jax.numpy as jnp
from jax import lax
from jax.experimental import pallas as pl
from jax.experimental.pallas import tpu as pltpu
from jax.sharding import Mesh
from jax.sharding import PartitionSpec as P

PROBES = 8
LEVELS = 256
NX, NW, NY = 4, 8, 128
NZ = 4 * NW
PITCH = NZ + 8
GX = ("xa", "xb")
GY = ("ya", "yb")
GZ = ("za", "zb")
REST = GX + GZ
EVERY = GX + GY + GZ

disorder_width = 4.0
spectral_scale = 8.4
TWO = 2.0 / spectral_scale
E_MUL = TWO * disorder_width / LEVELS
E_ADD = TWO * disorder_width * (0.5 / LEVELS - 0.5)

PLANES = 18
ROWS = 24
FRACTION = 2.0**20
SMALL = pltpu.CompilerParams(vmem_limit_bytes=24 * 1024 * 1024)


def vmem(n):
    return [pl.BlockSpec(memory_space=pltpu.VMEM)] * n


def lanes(shape):
    return lax.broadcasted_iota(jnp.int32, shape, len(shape) - 1)


def face_kernel(bits_far, levels_far, even, odd, bits, levels, done):
    copies = [
        pltpu.make_async_copy(bits_far, bits, done.at[0]),
        pltpu.make_async_copy(levels_far, levels, done.at[1]),
    ]
    for copy in copies:
        copy.start()
    for copy in copies:
        copy.wait()
    upper = lax.axis_index("xb")
    for out, first in ((even, 1 - upper), (odd, upper)):
        for i in range(3):
            out[8 * i : 8 * i + 8] = bits[first + i]
        for i in range(2):
            out[24 + 8 * i : 32 + 8 * i] = levels[2 * first + i]


def plane_list(bits, levels, below, above):
    found = []
    for x in range(-3, 7):
        if x < 0:
            found.append((below, 8 * (x + 3)))
        elif x < NX:
            found.append((bits, x))
        else:
            found.append((above, 8 * (x - 4)))
    for x in range(-2, 6):
        if x < 0:
            found.append((below, 24 + 8 * (x + 2)))
        elif x < NX:
            found.append((levels, x))
        else:
            found.append((above, 24 + 8 * (x - 4)))
    return found


def plane_tile(plane):
    ref, at = plane
    if len(ref.shape) == 3:
        return ref[at]
    return ref[at : at + NW, :]


def word_row(plane, w):
    ref, at = plane
    if len(ref.shape) == 3:
        return ref[at, w : w + 1, :]
    return ref[at + w : at + w + 1, :]


def level_kernel(bits, levels, even, odd, below, above, z_even, z_odd, low, high):
    upper = lax.axis_index("xb")
    near, far = even[pl.ds(40 * (1 - upper), 40), :], odd[...]
    below[...] = jnp.where(upper == 1, near, far)
    above[...] = jnp.where(upper == 1, far, near)
    planes = plane_list(bits, levels, below, above)
    for out, w in ((low, 0), (high, NW - 1)):
        out[16:24] = jnp.zeros((8, NY), jnp.int32)
        for k, plane in enumerate(planes):
            out[k : k + 1] = word_row(plane, w)
    up = lax.axis_index("zb") == 0
    z_even[...] = jnp.where(up, high[...], low[...])
    z_odd[...] = jnp.where(up, low[...], high[...])


def tiles():
    tile = (PROBES, NY)
    probe = lax.broadcasted_iota(jnp.int32, tile, 0)
    return tile, probe, lanes(tile), [jnp.left_shift(1, 4 * probe + j) for j in range(4)]


def sign_of(row, bit):
    return jnp.where((row & bit) != 0, 1.0, -1.0)


def energy_of(row, j):
    return (jnp.right_shift(row, 8 * j) & 255).astype(jnp.float32) * E_MUL + E_ADD


def step(v, energy, at, place):
    x, z = at
    own = v[x, z]
    s = pltpu.roll(own, NY - 1, 1) + pltpu.roll(own, 1, 1)
    s = s + (v[x + 1, z] + v[x - 1, z])
    s = s + (v[x, z + 1] + v[x, z - 1])
    return energy[place] * own - TWO * s


def sums_row(sums, mask, probe, lane):
    row = jnp.zeros(lane.shape, jnp.float32)
    for n, acc in enumerate(sums):
        total = jnp.sum(jnp.where(mask, acc, 0.0), axis=1, keepdims=True)
        row = jnp.where(lane == 8 * n + probe, total, row)
    return jnp.sum(row, axis=0, keepdims=True)


def add_sums(sums, v0, x, z, values):
    sign = v0[x + 3, z + 3]
    return [acc + sign * v for acc, v in zip(sums, values)]


def inner_kernel(bits, levels, below, above, strips, sums_out, v0, energy, v1, v2, v3):
    planes = plane_list(bits, levels, below, above)
    tile, probe, lane, bit_of = tiles()
    word = lax.broadcasted_iota(jnp.int32, tile, 0)
    mask = (lane // 16 == word) & (lane % 16 < 12)
    strips[16:24] = jnp.zeros((8, NY), jnp.int32)
    for k, plane in enumerate(planes):
        rolled = pltpu.roll(plane_tile(plane), 6, 1, stride=16, stride_axis=0)
        strips[k : k + 1] = jnp.sum(jnp.where(mask, rolled, 0), axis=0, keepdims=True)

    for w in range(NW):
        for k in range(10):
            row = jnp.broadcast_to(word_row(planes[k], w), tile)
            for j in range(4):
                v0[k, 4 * w + j + 3] = sign_of(row, bit_of[j])
        for k in range(8):
            row = jnp.broadcast_to(word_row(planes[10 + k], w), tile)
            for j in range(4):
                energy[k, 4 * w + j + 2] = energy_of(row, j)

    def first(i, carry):
        for u in range(2):
            x = 2 * i + u
            for z in range(3, NZ + 1):
                v1[x, z] = 0.5 * step(v0, energy, (x + 1, z + 1), (x, z))
        return carry

    lax.fori_loop(0, (NX + 4) // 2, first, 0)

    def second(i, carry):
        for u in range(2):
            x = 2 * i + u
            for z in range(3, NZ - 1):
                v2[x, z] = step(v1, energy, (x + 1, z + 1), (x + 1, z + 1)) - v0[x + 2, z + 2]
        return carry

    lax.fori_loop(0, (NX + 2) // 2, second, 0)

    def third(i, sums):
        for u in range(2):
            x = 2 * i + u
            for z in range(3, NZ - 3):
                one = v1[x + 2, z + 2]
                two = v2[x + 1, z + 1]
                three = step(v2, energy, (x + 1, z + 1), (x + 2, z + 2)) - one
                v3[x, z] = three
                sums = add_sums(sums, v0, x, z, (one, two, three))
        return tuple(sums)

    sums = lax.fori_loop(0, NX // 2, third, (jnp.zeros(tile, jnp.float32),) * 3)
    for n in range(3):
        sums_out[n] = sums[n]


def outer_kernel(
    z_odd, z_even, strips_in, sums_in, v0_in, energy_in, v1_in, v2_in, v3_in,
    strips, v0, energy, v1, v2, v3,
    under, over,
):
    up = lax.axis_index("zb") == 0
    under[...] = jnp.where(up, z_odd[...], z_even[...])
    over[...] = jnp.where(up, z_even[...], z_odd[...])
    del v0_in, energy_in, v1_in, v2_in, v3_in
    tile, probe, lane, bit_of = tiles()
    strips[:ROWS] = strips_in[...]
    wide = lanes((ROWS, NY))
    strips[ROWS:] = jnp.where(
        wide < 16, pltpu.roll(under[...], 6, 1), pltpu.roll(over[...], 6 + 112, 1)
    )
    for ref, base in ((under, -4), (over, NZ)):
        for k in range(10):
            row = jnp.broadcast_to(ref[k : k + 1, :], tile)
            for j in range(4):
                if -3 <= base + j < NZ + 3:
                    v0[k, base + j + 3] = sign_of(row, bit_of[j])
        for k in range(8):
            row = jnp.broadcast_to(ref[10 + k : 11 + k, :], tile)
            for j in range(4):
                if -2 <= base + j < NZ + 2:
                    energy[k, base + j + 2] = energy_of(row, j)
    for x in range(NX + 4):
        for z in (0, 1, 2, NZ + 1, NZ + 2, NZ + 3):
            v1[x, z] = 0.5 * step(v0, energy, (x + 1, z + 1), (x, z))
    for x in range(NX + 2):
        for z in (0, 1, 2, NZ - 1, NZ, NZ + 1):
            v2[x, z] = step(v1, energy, (x + 1, z + 1), (x + 1, z + 1)) - v0[x + 2, z + 2]
    sums = [sums_in[n] for n in range(3)]
    for x in range(NX):
        for z in (0, 1, 2, NZ - 3, NZ - 2, NZ - 1):
            one = v1[x + 2, z + 2]
            two = v2[x + 1, z + 1]
            three = step(v2, energy, (x + 1, z + 1), (x + 2, z + 2)) - one
            v3[x, z] = three
            sums = add_sums(sums, v0, x, z, (one, two, three))
    row = sums_row(sums, (lane >= 3) & (lane < NY - 3), probe, lane)
    whole = row.astype(jnp.int32)
    part = (row - whole.astype(jnp.float32)) * FRACTION
    strips[PLANES : PLANES + 1] = whole
    strips[PLANES + 1 : PLANES + 2] = part.astype(jnp.int32)


def edge_kernel(
    gathered, v2, v3,
    previous, current, message,
    words, e0, energy, e1, e2, e3, partial, blocks, done,
):
    count = gathered.shape[0] // (2 * ROWS)
    tile, probe, lane, bit_of = tiles()
    wide = lanes((ROWS, NY))

    place = 2 * lax.axis_index("ya") + lax.axis_index("yb")
    first = place + count - 1

    def interfaces(i, carry):
        for u in range(2):
            k = (first + 2 * i + u) % count
            here, there = 2 * ROWS * k, 2 * ROWS * ((k + 1) % count)
            left = wide % 16 < 6
            own = jnp.where(left, gathered[pl.ds(here, ROWS), :], gathered[pl.ds(there, ROWS), :])
            far = jnp.where(
                left,
                gathered[pl.ds(here + ROWS, ROWS), :],
                gathered[pl.ds(there + ROWS, ROWS), :],
            )
            words[u, 0] = jnp.where(wide < 16, far, pltpu.roll(own, 16, 1))
            words[u, 1] = own
            words[u, 2] = jnp.where(wide >= 112, far, pltpu.roll(own, 112, 1))
        for u in range(2):
            for n in range(3):
                for k in range(10):
                    row = jnp.broadcast_to(words[u, n, k : k + 1, :], tile)
                    for j in range(4):
                        z = 4 * n - 4 + j
                        if -3 <= z < 7:
                            e0[u, k, z + 3] = sign_of(row, bit_of[j])
                for k in range(8):
                    row = jnp.broadcast_to(words[u, n, 10 + k : 11 + k, :], tile)
                    for j in range(4):
                        z = 4 * n - 4 + j
                        if -2 <= z < 6:
                            energy[u, k, z + 2] = energy_of(row, j)
        for u in range(2):
            for x in range(8):
                for z in range(8):
                    e1[u, x, z] = 0.5 * step(e0.at[u], energy.at[u], (x + 1, z + 1), (x, z))
        for u in range(2):
            for x in range(6):
                for z in range(6):
                    e2[2 * i + u, x, z] = (
                        step(e1.at[u], energy.at[u], (x + 1, z + 1), (x + 1, z + 1))
                        - e0[u, x + 2, z + 2]
                    )
        for u in range(2):
            sums = (jnp.zeros(tile, jnp.float32),) * 3
            for x in range(4):
                for z in range(4):
                    one = e1[u, x + 2, z + 2]
                    two = e2[2 * i + u, x + 1, z + 1]
                    three = (
                        step(e2.at[2 * i + u], energy.at[u], (x + 1, z + 1), (x + 2, z + 2)) - one
                    )
                    e3[2 * i + u, x, z] = three
                    sums = add_sums(sums, e0.at[u], x, z, (one, two, three))
            for n in range(3):
                partial[(first + 2 * i + u) % count, n] = sums[n]

        @pl.when(i == 0)
        def _():
            lax.fori_loop(0, NX, merge, 0)

        return carry

    right = lane % 16 < 6
    outside = (lane < 3) | (lane >= NY - 3)
    rows = blocks.reshape(2 * NX * PROBES * PITCH, NY)

    def copy_out(n, x):
        return pltpu.make_async_copy(
            blocks.at[n, x, :, pl.ds(0, NZ), :], (previous, current)[n].at[:, x], done.at[n, x]
        )

    def merge(x, carry):
        for n, (main, edge, margin) in enumerate(((v2, e2, 1), (v3, e3, 0))):
            for j in range(4):
                fix = jnp.where(
                    right,
                    edge[1, x + margin, j + margin],
                    edge[0, x + margin, j + margin],
                )
                for w in range(NW):
                    z = 4 * w + j
                    moved = pltpu.roll(fix, (-16 * w - 6) % NY, 1)
                    value = jnp.where(outside, moved, main[x + margin, z + margin])
                    at = (n * NX + x) * PROBES * PITCH + z
                    rows[pl.ds(at, PROBES, stride=PITCH), :] = value
            copy_out(n, x).start()
        return carry

    lax.fori_loop(0, count // 2, interfaces, 0)
    sums = [sum((partial[k, n] for k in range(1, count)), partial[0, n]) for n in range(3)]
    row = sums_row(sums, (lane % 16 >= 3) & (lane % 16 < 9), probe, lane)
    for k in range(count):
        at = 2 * ROWS * k + PLANES
        whole = gathered[at : at + 1, :].astype(jnp.float32)
        part = gathered[at + 1 : at + 2, :].astype(jnp.float32)
        row = row + (whole + part * (1.0 / FRACTION))
    message[...] = jnp.broadcast_to(row, message.shape)
    for n in range(2):
        for x in range(NX):
            copy_out(n, x).wait()


def moment_kernel(parts, moments, *, scale):
    row = jnp.sum(parts[...], axis=0, keepdims=True) * scale
    for n in range(3):
        moments[n : n + 1, :] = pltpu.roll(row, (-8 * n) % NY, 1)[:, :PROBES]


def local(rows, dtype=jnp.int32):
    return pltpu.VMEM(rows, dtype)


def keep(array):
    return pltpu.with_memory_space_constraint(array, pltpu.VMEM)


def far(array):
    return pltpu.with_memory_space_constraint(array, pltpu.HBM)


def across(axis):
    size = lax.axis_size(axis)
    return [(i, (i + 1) % size if i % 2 else (i - 1) % size) for i in range(size)]


def groups():
    sizes = [lax.axis_size(axis) for axis in EVERY]
    found = {}
    for index, (xa, xb, ya, yb, za, zb) in enumerate(itertools.product(*map(range, sizes))):
        found.setdefault(((ya + zb) % sizes[2], yb), []).append(
            (((2 * xa + xb + za) % sizes[4], xa, xb, zb), index)
        )
    return [[index for _, index in sorted(members)] for members in found.values()]


def per_device(bits, levels):
    f32 = jnp.float32
    face = (40, NY)
    even, odd, bits, levels = pl.pallas_call(
        face_kernel,
        out_shape=(local(face), local(face), local(bits.shape), local(levels.shape)),
        in_specs=[pl.BlockSpec(memory_space=pltpu.HBM)] * 2,
        out_specs=tuple(vmem(4)),
        scratch_shapes=[pltpu.SemaphoreType.DMA((2,))],
        name="face",
        compiler_params=SMALL,
    )(far(bits), far(levels))
    bits, levels = keep(bits), keep(levels)
    odd = keep(lax.ppermute(odd, GX, across(GX)))
    even = keep(lax.all_gather(even, "xb", tiled=True))
    below, above, z_even, z_odd = pl.pallas_call(
        level_kernel,
        out_shape=(local(face),) * 2 + (local((ROWS, NY)),) * 2,
        in_specs=vmem(4),
        out_specs=tuple(vmem(4)),
        scratch_shapes=[pltpu.VMEM((ROWS, NY), jnp.int32)] * 2,
        name="level",
        compiler_params=SMALL,
    )(bits, levels, even, odd)
    z_odd = keep(lax.ppermute(z_odd, GZ, across(GZ)))
    z_even = keep(lax.ppermute(z_even, "zb", [(0, 1), (1, 0)]))

    def field(margin):
        return local((NX + 2 * margin, NZ + 2 * margin, PROBES, NY), f32)

    fields = [field(margin) for margin in (3, 2, 2, 1, 0)]
    strips, *inner = pl.pallas_call(
        inner_kernel,
        out_shape=(local((ROWS, NY)), local((3, PROBES, NY), f32), *fields),
        in_specs=vmem(4),
        out_specs=tuple(vmem(7)),
        name="inner",
        compiler_params=SMALL,
    )(bits, levels, keep(below), keep(above))
    inner = [keep(array) for array in (strips, *inner)]
    strips, *_, v2, v3 = pl.pallas_call(
        outer_kernel,
        out_shape=(local((2 * ROWS, NY)), *fields),
        in_specs=vmem(9),
        out_specs=tuple(vmem(6)),
        input_output_aliases={4 + i: 1 + i for i in range(5)},
        scratch_shapes=[pltpu.VMEM((ROWS, NY), jnp.int32)] * 2,
        name="outer",
        compiler_params=SMALL,
    )(z_odd, z_even, *inner)
    gathered = keep(lax.all_gather(strips, GY, tiled=True))
    count = lax.axis_size(GY)
    rest = lax.axis_size(REST)
    total = rest * count * NX * NZ * NY
    block = (PROBES, NX, NZ, NY)
    hbm = pl.BlockSpec(memory_space=pl.ANY)

    def edge(n, margin):
        return pltpu.VMEM((n, 4 + 2 * margin, 4 + 2 * margin, PROBES, NY), f32)

    previous, current, message = pl.pallas_call(
        edge_kernel,
        out_shape=(
            jax.ShapeDtypeStruct(block, f32),
            jax.ShapeDtypeStruct(block, f32),
            local((rest, NY), f32),
        ),
        in_specs=vmem(3),
        out_specs=(hbm, hbm, vmem(1)[0]),
        scratch_shapes=[
            pltpu.VMEM((2, 3, ROWS, NY), jnp.int32),
            edge(2, 3),
            edge(2, 2),
            edge(2, 2),
            edge(count, 1),
            edge(count, 0),
            pltpu.VMEM((count, 3, PROBES, NY), f32),
            pltpu.VMEM((2, NX, PROBES, PITCH, NY), f32),
            pltpu.SemaphoreType.DMA((2, NX)),
        ],
        name="edges",
        compiler_params=SMALL,
    )(gathered, keep(v2), keep(v3))
    parts = lax.all_to_all(message, EVERY, 0, 0, axis_index_groups=groups(), tiled=True)
    moments = pl.pallas_call(
        functools.partial(moment_kernel, scale=1.0 / total),
        out_shape=jax.ShapeDtypeStruct((3, PROBES), f32),
        in_specs=vmem(1),
        out_specs=vmem(1)[0],
        name="moment",
        compiler_params=SMALL,
    )(keep(parts))
    return moments, previous, current


def solution(mesh):
    halves = [n for axis in ("gx", "gy", "gz") for n in (mesh.shape[axis] // 2, 2)]
    torus = Mesh(mesh.devices.reshape(halves), GX + GY + GZ)
    return jax.shard_map(
        per_device,
        mesh=torus,
        in_specs=(P(GX, GZ, GY), P(GX, GZ, GY)),
        out_specs=(P(), P(None, GX, GZ, GY), P(None, GX, GZ, GY)),
        check_vma=False,
    )
```

```python
import functools
import itertools

import jax
import jax.numpy as jnp
from jax import lax
from jax.experimental import pallas as pl
from jax.experimental.pallas import tpu as pltpu
from jax.sharding import Mesh
from jax.sharding import PartitionSpec as P

PROBES = 8
LEVELS = 256
NX, NW, NY = 4, 8, 128
NZ = 4 * NW
PITCH = NZ + 8
GX = ("xa", "xb")
GY = ("ya", "yb")
GZ = ("za", "zb")
REST = GX + GZ
EVERY = GX + GY + GZ

disorder_width = 4.0
spectral_scale = 8.4
TWO = 2.0 / spectral_scale
E_MUL = TWO * disorder_width / LEVELS
E_ADD = TWO * disorder_width * (0.5 / LEVELS - 0.5)

PLANES = 18
ROWS = 24
FRACTION = 2.0**20
SMALL = pltpu.CompilerParams(vmem_limit_bytes=24 * 1024 * 1024)


def vmem(n):
    return [pl.BlockSpec(memory_space=pltpu.VMEM)] * n


def lanes(shape):
    return lax.broadcasted_iota(jnp.int32, shape, len(shape) - 1)


def face_kernel(bits_far, levels_far, even, odd, bits, levels, done):
    copies = [
        pltpu.make_async_copy(bits_far, bits, done.at[0]),
        pltpu.make_async_copy(levels_far, levels, done.at[1]),
    ]
    for copy in copies:
        copy.start()
    for copy in copies:
        copy.wait()
    upper = lax.axis_index("xb")
    for out, first in ((even, 1 - upper), (odd, upper)):
        for i in range(3):
            out[8 * i : 8 * i + 8] = bits[first + i]
        for i in range(2):
            out[24 + 8 * i : 32 + 8 * i] = levels[2 * first + i]


def plane_list(bits, levels, below, above):
    found = []
    for x in range(-3, 7):
        if x < 0:
            found.append((below, 8 * (x + 3)))
        elif x < NX:
            found.append((bits, x))
        else:
            found.append((above, 8 * (x - 4)))
    for x in range(-2, 6):
        if x < 0:
            found.append((below, 24 + 8 * (x + 2)))
        elif x < NX:
            found.append((levels, x))
        else:
            found.append((above, 24 + 8 * (x - 4)))
    return found


def plane_tile(plane):
    ref, at = plane
    if len(ref.shape) == 3:
        return ref[at]
    return ref[at : at + NW, :]


def word_row(plane, w):
    ref, at = plane
    if len(ref.shape) == 3:
        return ref[at, w : w + 1, :]
    return ref[at + w : at + w + 1, :]


def level_kernel(bits, levels, even, odd, below, above, z_even, z_odd, low, high):
    upper = lax.axis_index("xb")
    near, far = even[pl.ds(40 * (1 - upper), 40), :], odd[...]
    below[...] = jnp.where(upper == 1, near, far)
    above[...] = jnp.where(upper == 1, far, near)
    planes = plane_list(bits, levels, below, above)
    for out, w in ((low, 0), (high, NW - 1)):
        out[16:24] = jnp.zeros((8, NY), jnp.int32)
        for k, plane in enumerate(planes):
            out[k : k + 1] = word_row(plane, w)
    up = lax.axis_index("zb") == 0
    z_even[...] = jnp.where(up, high[...], low[...])
    z_odd[...] = jnp.where(up, low[...], high[...])


def tiles():
    tile = (PROBES, NY)
    probe = lax.broadcasted_iota(jnp.int32, tile, 0)
    return tile, probe, lanes(tile), [jnp.left_shift(1, 4 * probe + j) for j in range(4)]


def sign_of(row, bit):
    return jnp.where((row & bit) != 0, 1.0, -1.0)


def energy_of(row, j):
    return (jnp.right_shift(row, 8 * j) & 255).astype(jnp.float32) * E_MUL + E_ADD


def step(v, energy, at, place):
    x, z = at
    own = v[x, z]
    s = pltpu.roll(own, NY - 1, 1) + pltpu.roll(own, 1, 1)
    s = s + (v[x + 1, z] + v[x - 1, z])
    s = s + (v[x, z + 1] + v[x, z - 1])
    return energy[place] * own - TWO * s


def sums_row(sums, mask, probe, lane):
    row = jnp.zeros(lane.shape, jnp.float32)
    for n, acc in enumerate(sums):
        total = jnp.sum(jnp.where(mask, acc, 0.0), axis=1, keepdims=True)
        row = jnp.where(lane == 8 * n + probe, total, row)
    return jnp.sum(row, axis=0, keepdims=True)


def add_sums(sums, v0, x, z, values):
    sign = v0[x + 3, z + 3]
    return [acc + sign * v for acc, v in zip(sums, values)]


def inner_kernel(bits, levels, below, above, strips, sums_out, v0, energy, v1, v2, v3):
    planes = plane_list(bits, levels, below, above)
    tile, probe, lane, bit_of = tiles()
    word = lax.broadcasted_iota(jnp.int32, tile, 0)
    mask = (lane // 16 == word) & (lane % 16 < 12)
    strips[16:24] = jnp.zeros((8, NY), jnp.int32)
    for k, plane in enumerate(planes):
        rolled = pltpu.roll(plane_tile(plane), 6, 1, stride=16, stride_axis=0)
        strips[k : k + 1] = jnp.sum(jnp.where(mask, rolled, 0), axis=0, keepdims=True)

    for w in range(NW):
        for k in range(10):
            row = jnp.broadcast_to(word_row(planes[k], w), tile)
            for j in range(4):
                v0[k, 4 * w + j + 3] = sign_of(row, bit_of[j])
        for k in range(8):
            row = jnp.broadcast_to(word_row(planes[10 + k], w), tile)
            for j in range(4):
                energy[k, 4 * w + j + 2] = energy_of(row, j)

    def first(i, carry):
        for u in range(4):
            x = 4 * i + u
            for z in range(3, NZ + 1):
                v1[x, z] = 0.5 * step(v0, energy, (x + 1, z + 1), (x, z))
        return carry

    lax.fori_loop(0, (NX + 4) // 4, first, 0)

    def second(i, carry):
        for u in range(3):
            x = 3 * i + u
            for z in range(3, NZ - 1):
                v2[x, z] = step(v1, energy, (x + 1, z + 1), (x + 1, z + 1)) - v0[x + 2, z + 2]
        return carry

    lax.fori_loop(0, (NX + 2) // 3, second, 0)

    def third(i, sums):
        for u in range(4):
            x = 4 * i + u
            for z in range(3, NZ - 3):
                one = v1[x + 2, z + 2]
                two = v2[x + 1, z + 1]
                three = step(v2, energy, (x + 1, z + 1), (x + 2, z + 2)) - one
                v3[x, z] = three
                sums = add_sums(sums, v0, x, z, (one, two, three))
        return tuple(sums)

    sums = lax.fori_loop(0, NX // 4, third, (jnp.zeros(tile, jnp.float32),) * 3)
    for n in range(3):
        sums_out[n] = sums[n]


def outer_kernel(
    z_odd, z_even, strips_in, sums_in, v0_in, energy_in, v1_in, v2_in, v3_in,
    strips, v0, energy, v1, v2, v3,
    under, over,
):
    up = lax.axis_index("zb") == 0
    under[...] = jnp.where(up, z_odd[...], z_even[...])
    over[...] = jnp.where(up, z_even[...], z_odd[...])
    del v0_in, energy_in, v1_in, v2_in, v3_in
    tile, probe, lane, bit_of = tiles()
    strips[:ROWS] = strips_in[...]
    wide = lanes((ROWS, NY))
    strips[ROWS:] = jnp.where(
        wide < 16, pltpu.roll(under[...], 6, 1), pltpu.roll(over[...], 6 + 112, 1)
    )
    for ref, base in ((under, -4), (over, NZ)):
        for k in range(10):
            row = jnp.broadcast_to(ref[k : k + 1, :], tile)
            for j in range(4):
                if -3 <= base + j < NZ + 3:
                    v0[k, base + j + 3] = sign_of(row, bit_of[j])
        for k in range(8):
            row = jnp.broadcast_to(ref[10 + k : 11 + k, :], tile)
            for j in range(4):
                if -2 <= base + j < NZ + 2:
                    energy[k, base + j + 2] = energy_of(row, j)
    for x in range(NX + 4):
        for z in (0, 1, 2, NZ + 1, NZ + 2, NZ + 3):
            v1[x, z] = 0.5 * step(v0, energy, (x + 1, z + 1), (x, z))
    for x in range(NX + 2):
        for z in (0, 1, 2, NZ - 1, NZ, NZ + 1):
            v2[x, z] = step(v1, energy, (x + 1, z + 1), (x + 1, z + 1)) - v0[x + 2, z + 2]
    sums = [sums_in[n] for n in range(3)]
    for x in range(NX):
        for z in (0, 1, 2, NZ - 3, NZ - 2, NZ - 1):
            one = v1[x + 2, z + 2]
            two = v2[x + 1, z + 1]
            three = step(v2, energy, (x + 1, z + 1), (x + 2, z + 2)) - one
            v3[x, z] = three
            sums = add_sums(sums, v0, x, z, (one, two, three))
    row = sums_row(sums, (lane >= 3) & (lane < NY - 3), probe, lane)
    whole = row.astype(jnp.int32)
    part = (row - whole.astype(jnp.float32)) * FRACTION
    strips[PLANES : PLANES + 1] = whole
    strips[PLANES + 1 : PLANES + 2] = part.astype(jnp.int32)


def edge_kernel(
    gathered, v2, v3,
    previous, current, message,
    words, e0, energy, e1, e2, e3, partial, blocks, done,
):
    count = gathered.shape[0] // (2 * ROWS)
    tile, probe, lane, bit_of = tiles()
    wide = lanes((ROWS, NY))

    place = 2 * lax.axis_index("ya") + lax.axis_index("yb")
    first = place + count - 1

    def interfaces(i, carry):
        for u in range(2):
            k = (first + 2 * i + u) % count
            here, there = 2 * ROWS * k, 2 * ROWS * ((k + 1) % count)
            left = wide % 16 < 6
            own = jnp.where(left, gathered[pl.ds(here, ROWS), :], gathered[pl.ds(there, ROWS), :])
            far = jnp.where(
                left,
                gathered[pl.ds(here + ROWS, ROWS), :],
                gathered[pl.ds(there + ROWS, ROWS), :],
            )
            words[u, 0] = jnp.where(wide < 16, far, pltpu.roll(own, 16, 1))
            words[u, 1] = own
            words[u, 2] = jnp.where(wide >= 112, far, pltpu.roll(own, 112, 1))
        for u in range(2):
            for n in range(3):
                for k in range(10):
                    row = jnp.broadcast_to(words[u, n, k : k + 1, :], tile)
                    for j in range(4):
                        z = 4 * n - 4 + j
                        if -3 <= z < 7:
                            e0[u, k, z + 3] = sign_of(row, bit_of[j])
                for k in range(8):
                    row = jnp.broadcast_to(words[u, n, 10 + k : 11 + k, :], tile)
                    for j in range(4):
                        z = 4 * n - 4 + j
                        if -2 <= z < 6:
                            energy[u, k, z + 2] = energy_of(row, j)
        for u in range(2):
            for x in range(8):
                for z in range(8):
                    e1[u, x, z] = 0.5 * step(e0.at[u], energy.at[u], (x + 1, z + 1), (x, z))
        for u in range(2):
            for x in range(6):
                for z in range(6):
                    e2[2 * i + u, x, z] = (
                        step(e1.at[u], energy.at[u], (x + 1, z + 1), (x + 1, z + 1))
                        - e0[u, x + 2, z + 2]
                    )
        for u in range(2):
            sums = (jnp.zeros(tile, jnp.float32),) * 3
            for x in range(4):
                for z in range(4):
                    one = e1[u, x + 2, z + 2]
                    two = e2[2 * i + u, x + 1, z + 1]
                    three = (
                        step(e2.at[2 * i + u], energy.at[u], (x + 1, z + 1), (x + 2, z + 2)) - one
                    )
                    e3[2 * i + u, x, z] = three
                    sums = add_sums(sums, e0.at[u], x, z, (one, two, three))
            for n in range(3):
                partial[(first + 2 * i + u) % count, n] = sums[n]

        @pl.when(i == 0)
        def _():
            lax.fori_loop(0, NX, merge, 0)

        return carry

    right = lane % 16 < 6
    outside = (lane < 3) | (lane >= NY - 3)
    rows = blocks.reshape(2 * NX * PROBES * PITCH, NY)

    def copy_out(n, x):
        return pltpu.make_async_copy(
            blocks.at[n, x, :, pl.ds(0, NZ), :], (previous, current)[n].at[:, x], done.at[n, x]
        )

    def merge(x, carry):
        for n, (main, edge, margin) in enumerate(((v2, e2, 1), (v3, e3, 0))):
            for j in range(4):
                fix = jnp.where(
                    right,
                    edge[1, x + margin, j + margin],
                    edge[0, x + margin, j + margin],
                )
                for w in range(NW):
                    z = 4 * w + j
                    moved = pltpu.roll(fix, (-16 * w - 6) % NY, 1)
                    value = jnp.where(outside, moved, main[x + margin, z + margin])
                    at = (n * NX + x) * PROBES * PITCH + z
                    rows[pl.ds(at, PROBES, stride=PITCH), :] = value
            copy_out(n, x).start()
        return carry

    lax.fori_loop(0, count // 2, interfaces, 0)
    sums = [sum((partial[k, n] for k in range(1, count)), partial[0, n]) for n in range(3)]
    row = sums_row(sums, (lane % 16 >= 3) & (lane % 16 < 9), probe, lane)
    for k in range(count):
        at = 2 * ROWS * k + PLANES
        whole = gathered[at : at + 1, :].astype(jnp.float32)
        part = gathered[at + 1 : at + 2, :].astype(jnp.float32)
        row = row + (whole + part * (1.0 / FRACTION))
    message[...] = jnp.broadcast_to(row, message.shape)
    for n in range(2):
        for x in range(NX):
            copy_out(n, x).wait()


def moment_kernel(parts, moments, *, scale):
    row = jnp.sum(parts[...], axis=0, keepdims=True) * scale
    for n in range(3):
        moments[n : n + 1, :] = pltpu.roll(row, (-8 * n) % NY, 1)[:, :PROBES]


def local(rows, dtype=jnp.int32):
    return pltpu.VMEM(rows, dtype)


def keep(array):
    return pltpu.with_memory_space_constraint(array, pltpu.VMEM)


def far(array):
    return pltpu.with_memory_space_constraint(array, pltpu.HBM)


def across(axis):
    size = lax.axis_size(axis)
    return [(i, (i + 1) % size if i % 2 else (i - 1) % size) for i in range(size)]


def groups():
    sizes = [lax.axis_size(axis) for axis in EVERY]
    found = {}
    for index, (xa, xb, ya, yb, za, zb) in enumerate(itertools.product(*map(range, sizes))):
        found.setdefault(((ya + zb) % sizes[2], yb), []).append(
            (((2 * xa + xb + za) % sizes[4], xa, xb, zb), index)
        )
    return [[index for _, index in sorted(members)] for members in found.values()]


def per_device(bits, levels):
    f32 = jnp.float32
    face = (40, NY)
    even, odd, bits, levels = pl.pallas_call(
        face_kernel,
        out_shape=(local(face), local(face), local(bits.shape), local(levels.shape)),
        in_specs=[pl.BlockSpec(memory_space=pltpu.HBM)] * 2,
        out_specs=tuple(vmem(4)),
        scratch_shapes=[pltpu.SemaphoreType.DMA((2,))],
        name="face",
        compiler_params=SMALL,
    )(far(bits), far(levels))
    bits, levels = keep(bits), keep(levels)
    odd = keep(lax.ppermute(odd, GX, across(GX)))
    even = keep(lax.all_gather(even, "xb", tiled=True))
    below, above, z_even, z_odd = pl.pallas_call(
        level_kernel,
        out_shape=(local(face),) * 2 + (local((ROWS, NY)),) * 2,
        in_specs=vmem(4),
        out_specs=tuple(vmem(4)),
        scratch_shapes=[pltpu.VMEM((ROWS, NY), jnp.int32)] * 2,
        name="level",
        compiler_params=SMALL,
    )(bits, levels, even, odd)
    z_odd = keep(lax.ppermute(z_odd, GZ, across(GZ)))
    z_even = keep(lax.ppermute(z_even, "zb", [(0, 1), (1, 0)]))

    def field(margin):
        return local((NX + 2 * margin, NZ + 2 * margin, PROBES, NY), f32)

    fields = [field(margin) for margin in (3, 2, 2, 1, 0)]
    strips, *inner = pl.pallas_call(
        inner_kernel,
        out_shape=(local((ROWS, NY)), local((3, PROBES, NY), f32), *fields),
        in_specs=vmem(4),
        out_specs=tuple(vmem(7)),
        name="inner",
        compiler_params=SMALL,
    )(bits, levels, keep(below), keep(above))
    inner = [keep(array) for array in (strips, *inner)]
    strips, *_, v2, v3 = pl.pallas_call(
        outer_kernel,
        out_shape=(local((2 * ROWS, NY)), *fields),
        in_specs=vmem(9),
        out_specs=tuple(vmem(6)),
        input_output_aliases={4 + i: 1 + i for i in range(5)},
        scratch_shapes=[pltpu.VMEM((ROWS, NY), jnp.int32)] * 2,
        name="outer",
        compiler_params=SMALL,
    )(z_odd, z_even, *inner)
    gathered = keep(lax.all_gather(strips, GY, tiled=True))
    count = lax.axis_size(GY)
    rest = lax.axis_size(REST)
    total = rest * count * NX * NZ * NY
    block = (PROBES, NX, NZ, NY)
    hbm = pl.BlockSpec(memory_space=pl.ANY)

    def edge(n, margin):
        return pltpu.VMEM((n, 4 + 2 * margin, 4 + 2 * margin, PROBES, NY), f32)

    previous, current, message = pl.pallas_call(
        edge_kernel,
        out_shape=(
            jax.ShapeDtypeStruct(block, f32),
            jax.ShapeDtypeStruct(block, f32),
            local((rest, NY), f32),
        ),
        in_specs=vmem(3),
        out_specs=(hbm, hbm, vmem(1)[0]),
        scratch_shapes=[
            pltpu.VMEM((2, 3, ROWS, NY), jnp.int32),
            edge(2, 3),
            edge(2, 2),
            edge(2, 2),
            edge(count, 1),
            edge(count, 0),
            pltpu.VMEM((count, 3, PROBES, NY), f32),
            pltpu.VMEM((2, NX, PROBES, PITCH, NY), f32),
            pltpu.SemaphoreType.DMA((2, NX)),
        ],
        name="edges",
        compiler_params=SMALL,
    )(gathered, keep(v2), keep(v3))
    parts = lax.all_to_all(message, EVERY, 0, 0, axis_index_groups=groups(), tiled=True)
    moments = pl.pallas_call(
        functools.partial(moment_kernel, scale=1.0 / total),
        out_shape=jax.ShapeDtypeStruct((3, PROBES), f32),
        in_specs=vmem(1),
        out_specs=vmem(1)[0],
        name="moment",
        compiler_params=SMALL,
    )(keep(parts))
    return moments, previous, current


def solution(mesh):
    halves = [n for axis in ("gx", "gy", "gz") for n in (mesh.shape[axis] // 2, 2)]
    torus = Mesh(mesh.devices.reshape(halves), GX + GY + GZ)
    return jax.shard_map(
        per_device,
        mesh=torus,
        in_specs=(P(GX, GZ, GY), P(GX, GZ, GY)),
        out_specs=(P(), P(None, GX, GZ, GY), P(None, GX, GZ, GY)),
        check_vma=False,
    )
```
